128 devices in a mesh: expert: 2 (over x_hi), seq: 8 (over x_lo, z), fsdp: 8 (over y, core).
Axes of the slice: x: 4 (x_hi: 2, x_lo: 2; x = x_hi * 2 + x_lo), y: 4, z: 4, core: 2. Of those that a mesh axis runs over, the one named last changes fastest.
Arguments:
- queries: bfloat16 [16384, 5120], P(('expert', 'seq', 'fsdp')), parts along dimension 0, may hold values from -100 to 100
- keys: bfloat16 [16384, 5120], P(('expert', 'seq', 'fsdp')), parts along dimension 0, may hold values from -100 to 100
- values: bfloat16 [16384, 5120], P(('expert', 'seq', 'fsdp')), parts along dimension 0, may hold values from -6 to 6
- query_gain: float32 [10240], P('expert'), parts along dimension 0, may hold values from 1 to 3
- key_gain: float32 [10240], P('expert'), parts along dimension 0, may hold values from 1 to 3
- timestep: int32 [2], P('expert'), parts along dimension 0, may hold values from 0 to 999, as said below
- gate_base: float32 [10240], P('expert'), parts along dimension 0, may hold values from -3 to 3
- time_weight: float32 [512, 5120], P('expert'), parts along dimension 0, may hold values from -0.375 to 0.375
Outputs:
- attended: bfloat16 [16384, 5120], P(('expert', 'seq', 'fsdp')), parts along dimension 0
The draws below stay inside these ranges and needn't reach their ends.
There are 2 independent parts, one for each index of `expert`. The reference program is written for one: setup_inputs(seed, part) draws one part's arguments, and reference() takes and returns one part's arrays. A program takes and returns all parts, laid end to end along the dimension named above; each array names one. Nothing has to cross between parts.
Inputs may be any that keep to these rules, and one draw needn't show every extreme that they name: Part 0 is the high-noise group, with a timestep from 875 to 999; part 1 the low-noise group, with one from 0 to 874.
All inputs are finite; a program needn't handle non-finite values.
Results may differ from the reference program's by a relative error of at most 0.012.
The reference program's roundings to bfloat16 on the way count: a program that leaves them out, or rounds other values in their place, can miss the bound.
Values may be sent and summed in bfloat16 or wider, within the bound.
No kernel may reach another device: no remote copies, remote signals or barrier semaphores. Data moves between devices by JAX's collectives and lax.ppermute only.
A program may use at most 384 MiB of HBM per device.

```python
import math
import jax
import jax.numpy as jnp
from jax import lax

D = 5120
HEADS = 40
HEAD_DIM = 128
FREQ = 256
HGT = 32
WID = 32
NSTEPS = 1000
BOUNDARY = 875
LENGTH = 8192


def noise_field(key, salt, row_total):
    drawn = jax.random.normal(jax.random.fold_in(key, salt), (row_total, D), jnp.float32)
    return jnp.clip(drawn, -6.0, 6.0)


def draw_queries(key, part):
    tensor = noise_field(key, 21, LENGTH)
    return tensor.astype(jnp.bfloat16)


def draw_keys(key, part):
    tensor = noise_field(key, 31, LENGTH)
    return tensor.astype(jnp.bfloat16)


def draw_timestep(key, part):
    upper_draw = jax.random.randint(jax.random.fold_in(key, 41), (1,), BOUNDARY, NSTEPS)
    lower_draw = jax.random.randint(jax.random.fold_in(key, 42), (1,), 0, BOUNDARY)
    return jnp.where(part == 0, upper_draw, lower_draw).astype(jnp.int32)


def block_levels(own_key, extent, cuts, smallest, largest):
    level = 1.0
    for dim, parts in cuts:
        steps = jax.random.uniform(jax.random.fold_in(jax.random.fold_in(own_key, 6), dim), (parts,), jnp.float32, smallest / len(cuts), largest / len(cuts))
        level = level * jnp.repeat(jnp.exp(steps), extent[dim] // parts).reshape((-1,) + (1,) * (len(extent) - 1 - dim))
    return level


def normal_values(own_key, extent, spread, bound, cuts=(), held_as=jnp.bfloat16):
    factor_of = block_levels(own_key, extent, cuts, -0.22, 0.18) if cuts else 1.0
    values = jax.random.normal(own_key, extent, jnp.float32) * spread * factor_of
    return jnp.minimum(jnp.maximum(values, -bound), bound).astype(held_as)


def setup_inputs(seed: int = 0, part: int = 0) -> dict:
    key_list = jax.random.split(jax.random.key(seed), 9)
    own_keys = jax.random.split(jax.random.fold_in(key_list[8], part), 9)
    queries = draw_queries(jax.random.fold_in(jax.random.fold_in(key_list[8], part), 71), part)
    keys = draw_keys(jax.random.fold_in(jax.random.fold_in(key_list[8], part), 71), part)
    values = normal_values(own_keys[2], (LENGTH, D), 1.0, 6.0, ((0, 64),))
    query_gain = jnp.clip(jax.random.uniform(own_keys[3], (D,), jnp.float32, 1.0, 3.0), 1.0, 3.0)
    key_gain = jnp.clip(jax.random.uniform(own_keys[4], (D,), jnp.float32, 1.0, 3.0), 1.0, 3.0)
    timestep = draw_timestep(jax.random.fold_in(jax.random.fold_in(key_list[8], part), 71), part)
    gate_base = normal_values(own_keys[6], (D,), 0.5, 3.0, (), jnp.float32)
    time_weight = normal_values(own_keys[7], (FREQ, D), FREQ ** -0.5, 0.375, (), jnp.float32)
    return {"queries": queries, "keys": keys, "values": values, "query_gain": query_gain, "key_gain": key_gain, "timestep": timestep, "gate_base": gate_base, "time_weight": time_weight}


EPSILON = 1e-06

def rms_normed(tensor, gain_vector):
    mean_square = lax.optimization_barrier(jnp.mean(tensor * tensor, axis=-1, keepdims=True))
    return tensor * lax.rsqrt(mean_square + EPSILON) * gain_vector

def rotate_pairs(tensor, positions):
    half_dim = HEAD_DIM // 2
    sixth = HEAD_DIM // 6
    frame_pairs = (HEAD_DIM - 4 * sixth) // 2
    pair_index = jnp.arange(half_dim, dtype=jnp.int32)
    in_frame = pair_index < frame_pairs
    in_height = (pair_index >= frame_pairs) & (pair_index < frame_pairs + sixth)
    local_index = jnp.where(in_frame, pair_index, jnp.where(in_height, pair_index - frame_pairs, pair_index - frame_pairs - sixth))
    segment_dims = jnp.where(in_frame, 2 * frame_pairs, 2 * sixth)
    inverse = jnp.power(jnp.float32(10000.0), -2.0 * local_index.astype(jnp.float32) / segment_dims.astype(jnp.float32))
    frame_at = positions // (HGT * WID)
    height_at = positions // WID % HGT
    width_at = positions % WID
    coordinate = jnp.where(in_frame[None, :], frame_at[:, None], jnp.where(in_height[None, :], height_at[:, None], width_at[:, None])).astype(jnp.float32)
    angle_table = coordinate * inverse[None, :]
    cosine = jnp.cos(angle_table)[:, None, :]
    sine_table = jnp.sin(angle_table)[:, None, :]
    paired = tensor.reshape(tensor.shape[0], tensor.shape[1], half_dim, 2)
    even_part = paired[..., 0]
    odd_part = paired[..., 1]
    turned = jnp.stack([even_part * cosine - odd_part * sine_table, even_part * sine_table + odd_part * cosine], axis=-1)
    return turned.reshape(tensor.shape)

def prepare(tensor, gain_vector, positions):
    normed = rms_normed(tensor.astype(jnp.float32), gain_vector)
    head_total = tensor.shape[1] // HEAD_DIM
    turned = rotate_pairs(normed.reshape(tensor.shape[0], head_total, HEAD_DIM), positions)
    return turned.reshape(tensor.shape).astype(jnp.bfloat16)

def gate_vector(timestep, base_slice, weight_slice):
    half_freq = FREQ // 2
    exponent = jnp.arange(half_freq, dtype=jnp.int32).astype(jnp.float32) / half_freq
    frequency = jnp.power(jnp.float32(10000.0), -exponent)
    phase = timestep.astype(jnp.float32)[:, None] * frequency[None, :]
    embedded = jnp.concatenate([jnp.cos(phase), jnp.sin(phase)], axis=1)
    projected = jnp.dot(embedded, weight_slice, precision=lax.Precision.HIGHEST, preferred_element_type=jnp.float32)
    return base_slice + projected[0]

def reference(queries, keys, values, query_gain, key_gain, timestep, gate_base, time_weight):
    positions = jnp.arange(LENGTH, dtype=jnp.int32)
    query_rot = prepare(queries, query_gain, positions).reshape(LENGTH, HEADS, HEAD_DIM)
    key_rot = prepare(keys, key_gain, positions).reshape(LENGTH, HEADS, HEAD_DIM)
    value_heads = values.reshape(LENGTH, HEADS, HEAD_DIM)
    score_scale = 1.0 / math.sqrt(HEAD_DIM)
    block_size = math.gcd(LENGTH, 1024)

    def one_head(head_index):
        head_query = lax.dynamic_index_in_dim(query_rot, head_index, 1, keepdims=False)
        head_key = lax.dynamic_index_in_dim(key_rot, head_index, 1, keepdims=False)
        head_value = lax.dynamic_index_in_dim(value_heads, head_index, 1, keepdims=False)
        query_blocks = head_query.reshape(LENGTH // block_size, block_size, HEAD_DIM)

        def one_block(query_block):
            scores = jnp.dot(query_block, head_key.T, preferred_element_type=jnp.float32) * score_scale
            row_peak = lax.optimization_barrier(jnp.max(scores, axis=1, keepdims=True))
            exponent_values = jnp.exp(scores - row_peak)
            weight_total = lax.optimization_barrier(jnp.sum(exponent_values, axis=1, keepdims=True))
            weights = exponent_values.astype(jnp.bfloat16)
            mixed_out = jnp.dot(weights, head_value, preferred_element_type=jnp.float32)
            return mixed_out / weight_total
        return lax.map(one_block, query_blocks).reshape(LENGTH, HEAD_DIM)
    per_head = lax.map(one_head, jnp.arange(HEADS, dtype=jnp.int32))
    heads_out = jnp.transpose(per_head, (1, 0, 2)).reshape(LENGTH, D)
    gate_full = gate_vector(timestep, gate_base, time_weight)
    return (heads_out * gate_full[None, :]).astype(jnp.bfloat16)
```

```python
import functools
import math

import jax
import jax.numpy as jnp
import numpy as np
from jax import lax
from jax.experimental import pallas as pl
from jax.experimental.pallas import tpu as pltpu
from jax.sharding import Mesh
from jax.sharding import PartitionSpec as P

HEAD_DIM = 128
FREQ = 256
HGT = 32
WID = 32
EPSILON = 1e-06
LOG2E = 1.4426950408889634
SCALE = LOG2E / math.sqrt(HEAD_DIM)
VMEM_BYTES = 63 * 1024 * 1024
F32 = jnp.float32
BF16 = jnp.bfloat16


def inverse_row():
    half = HEAD_DIM // 2
    sixth = HEAD_DIM // 6
    frame = (HEAD_DIM - 4 * sixth) // 2
    j = np.arange(half)
    in_frame = j < frame
    in_row = (j >= frame) & (j < frame + sixth)
    local = np.where(in_frame, j, np.where(in_row, j - frame, j - frame - sixth))
    dims = np.where(in_frame, 2 * frame, 2 * sixth)
    inverse = np.power(10000.0, -2.0 * local / dims).astype(np.float32)
    kind = np.where(in_frame, 0, np.where(in_row, 1, 2))
    return np.repeat(inverse, 2), np.repeat(kind, 2)


def prep_kernel(block_ref, inv_hbm, *refs, heads, plan, rotate):
    count = len(rotate) + 1
    steps = heads // 8
    sources, gains = refs[:count], refs[count:2 * count - 1]
    outs = refs[2 * count - 1:2 * count - 1 + len(plan)]
    scratch = refs[2 * count - 1 + len(plan):]
    inv_ref, swap_ref, cos_ref, sin_ref, sems = scratch[:5]
    bufs = scratch[5:5 + count]
    gain_bufs = scratch[5 + count:4 + 2 * count]
    rms_refs = scratch[4 + 2 * count:]
    tokens, width = bufs[0].shape
    step = pl.program_id(0)

    @pl.when(step == 0)
    def _():
        pairs = [(inv_hbm, inv_ref)] + list(zip(sources, bufs)) + list(zip(gains, gain_bufs))
        copies = [pltpu.make_async_copy(a, b, sems.at[n]) for n, (a, b) in enumerate(pairs)]
        for copy in copies:
            copy.start()
        lane = lax.broadcasted_iota(jnp.int32, (HEAD_DIM, HEAD_DIM), 1)
        depth = lax.broadcasted_iota(jnp.int32, (HEAD_DIM, HEAD_DIM), 0)
        below = jnp.where((lane % 2 == 0) & (depth == lane + 1), -1.0, 0.0)
        above = jnp.where((lane % 2 == 1) & (depth == lane - 1), 1.0, 0.0)
        swap_ref[...] = (below + above).astype(BF16)
        copies[0].wait()
        token = block_ref[0] * tokens + lax.broadcasted_iota(jnp.int32, (tokens, HEAD_DIM), 0)
        pair = lax.broadcasted_iota(jnp.int32, (tokens, HEAD_DIM), 1) // 2
        sixth = HEAD_DIM // 6
        frame_pairs = (HEAD_DIM - 4 * sixth) // 2
        frame = token // (HGT * WID)
        row = (token // WID) % HGT
        column = token % WID
        coord = jnp.where(pair < frame_pairs, frame,
                          jnp.where(pair < frame_pairs + sixth, row, column)).astype(F32)
        angle = coord * inv_ref[...]
        cos_ref[...] = jnp.cos(angle)
        sin_ref[...] = jnp.sin(angle)
        for copy in copies[1:]:
            copy.wait()
        for src, dst in zip(bufs, rms_refs):
            total = jnp.zeros((tokens, HEAD_DIM), F32)
            for h in range(width // HEAD_DIM):
                x = src[:, h * HEAD_DIM:(h + 1) * HEAD_DIM].astype(F32)
                total = total + x * x
            mean = jnp.sum(total, axis=1, keepdims=True) / width
            dst[...] = jnp.broadcast_to(lax.rsqrt(mean + EPSILON), (tokens, HEAD_DIM))

    even = lax.broadcasted_iota(jnp.int32, (1, HEAD_DIM), 1) % 2 == 0

    def rotated(n, head):
        x = bufs[n][:, pl.ds(pl.multiple_of(head * HEAD_DIM, HEAD_DIM), HEAD_DIM)]
        xs = jnp.dot(x, swap_ref[...], preferred_element_type=F32)
        g = gain_bufs[n][pl.ds(head, 1), :]
        gs = jnp.where(even, pltpu.roll(g, HEAD_DIM - 1, 1), pltpu.roll(g, 1, 1))
        r = rms_refs[n][...]
        return (x.astype(F32) * r * g) * cos_ref[...] + (xs * r * gs) * sin_ref[...]

    for dst, (first, slots) in zip(outs, plan):
        for slot in range(slots):
            head = first + step * slots + slot
            for n, turn in enumerate(rotate):
                y = rotated(n, head)
                dst[slot, n] = (y.T if turn else y).astype(BF16)
            v = bufs[-1][:, pl.ds(pl.multiple_of(head * HEAD_DIM, HEAD_DIM), HEAD_DIM)]
            dst[slot, count - 1] = v.astype(F32).T.astype(BF16)


def prepare(name, block, queries, keys, values, query_gain, key_gain, plan):
    tokens, width = queries.shape
    heads = width // HEAD_DIM
    inverse, _ = inverse_row()
    tile = (HEAD_DIM, tokens)
    hbm = pl.BlockSpec(memory_space=pltpu.HBM)
    rotate = (True, False)
    return pl.pallas_call(
        functools.partial(prep_kernel, heads=64, plan=plan, rotate=rotate),
        grid=(8,),
        in_specs=[pl.BlockSpec(memory_space=pltpu.SMEM)] + [hbm] * 6,
        out_specs=[pl.BlockSpec((slots, 3) + tile, lambda i: (i, 0, 0, 0))
                   for _, slots in plan],
        out_shape=[jax.ShapeDtypeStruct((8 * slots, 3) + tile, BF16) for _, slots in plan],
        scratch_shapes=[
            pltpu.VMEM((1, HEAD_DIM), F32),
            pltpu.VMEM((HEAD_DIM, HEAD_DIM), BF16),
            pltpu.VMEM((tokens, HEAD_DIM), F32),
            pltpu.VMEM((tokens, HEAD_DIM), F32),
            pltpu.SemaphoreType.DMA((6,)),
        ] + [pltpu.VMEM((tokens, width), BF16)] * 3
        + [pltpu.VMEM((heads, HEAD_DIM), F32)] * 2
        + [pltpu.VMEM((tokens, HEAD_DIM), F32)] * 2,
        compiler_params=pltpu.CompilerParams(vmem_limit_bytes=VMEM_BYTES),
        name=name,
    )(
        block,
        jnp.asarray(inverse)[None, :],
        queries,
        keys,
        values,
        query_gain.reshape(heads, HEAD_DIM),
        key_gain.reshape(heads, HEAD_DIM),
    )


def attend_kernel(*refs, sizes, first_has_query, resume, final, tk, sub):
    count = len(sizes)
    q_ref, gate_ref = refs[:2]
    pieces = refs[2:2 + count]
    at = 2 + count
    if resume:
        stat_in, mixed_in = refs[at:at + 2]
        at += 2
    if final:
        o_ref = refs[at]
        at += 1
    else:
        stat_out, mixed_out = refs[at:at + 2]
        at += 2
    k_buf, v_buf, s_buf, sems = refs[at:]

    @pl.when(pl.program_id(0) == 0)
    def _():
        copies = []
        offset = 0
        for i, size in enumerate(sizes):
            shift = 1 if (i == 0 and first_has_query) else 0
            for j, buf in enumerate((k_buf, v_buf)):
                copies.append(pltpu.make_async_copy(
                    pieces[i].at[:, shift + j], buf.at[pl.ds(offset, size)], sems.at[2 * i + j]))
            offset += size
        for copy in copies:
            copy.start()
        for copy in copies:
            copy.wait()

    tiles = q_ref.shape[0]
    tq = tiles * HEAD_DIM
    q = jnp.concatenate([q_ref[t, 0] for t in range(tiles)], axis=1).astype(F32) * SCALE
    q_high = q.astype(BF16)
    q_low = (q - q_high.astype(F32)).astype(BF16)
    q_both = jnp.concatenate([q_high, q_low], axis=0)
    blocks = sum(sizes) * HEAD_DIM // tk
    subs = tk // sub
    per_sub = sub // HEAD_DIM

    def scores(j, i):
        first = (j * subs + i) * per_sub
        k = k_buf[first:first + per_sub].reshape(sub, HEAD_DIM)
        s = jnp.dot(jnp.concatenate([k, k], axis=1), q_both, preferred_element_type=F32)
        s_buf[j % 2, i * sub:(i + 1) * sub, :] = s
        return jnp.max(s.reshape(sub // 8, 8, tq), axis=0)

    top = scores(0, 0)
    for i in range(1, subs):
        top = jnp.maximum(top, scores(0, i))
    if resume:
        peak = stat_in[0:1, :]
        total = stat_in[8:16, :]
        mixed = mixed_in[...]
    else:
        peak = jnp.full((1, tq), -1e30, F32)
        total = jnp.zeros((8, tq), F32)
        mixed = jnp.zeros((HEAD_DIM, tq), F32)
    for j in range(blocks):
        new_peak = jnp.maximum(peak, jnp.max(top, axis=0, keepdims=True))
        shrink = jnp.exp2(peak - new_peak)
        total = total * shrink
        part = None
        top = None
        for i in range(subs):
            if j + 1 < blocks:
                t = scores(j + 1, i)
                top = t if top is None else jnp.maximum(top, t)
            e = jnp.exp2(s_buf[j % 2, i * sub:(i + 1) * sub, :] - new_peak)
            total = total + jnp.sum(e.reshape(sub // 8, 8, tq), axis=0)
            first = (j * subs + i) * per_sub
            v = jnp.concatenate([v_buf[first + t] for t in range(per_sub)], axis=1)
            d = jnp.dot(v, e.astype(BF16), preferred_element_type=F32)
            part = d if part is None else part + d
        mixed = mixed * shrink + part
        peak = new_peak
    if final:
        out = mixed / jnp.sum(total, axis=0, keepdims=True)
        gate = gate_ref[...]
        for t in range(tiles):
            o_ref[t] = (out[:, t * HEAD_DIM:(t + 1) * HEAD_DIM] * gate).astype(BF16)
    else:
        stat_out[0:8, :] = jnp.broadcast_to(peak, (8, tq))
        stat_out[8:16, :] = total
        mixed_out[...] = mixed


def attend(name, own, gate, pieces, state=None, final=True, tq=512, tk=1024, sub=1024):
    sizes = tuple(p.shape[0] for p in pieces)
    query_tiles = own.shape[0]
    step = tq // HEAD_DIM
    keys = sum(sizes)
    state_specs = [pl.BlockSpec((16, tq), lambda i: (0, i)),
                   pl.BlockSpec((HEAD_DIM, tq), lambda i: (0, i))]
    state_shapes = [jax.ShapeDtypeStruct((16, query_tiles * HEAD_DIM), F32),
                    jax.ShapeDtypeStruct((HEAD_DIM, query_tiles * HEAD_DIM), F32)]
    out = pl.pallas_call(
        functools.partial(attend_kernel, sizes=sizes, first_has_query=pieces[0].shape[1] == 3,
                          resume=state is not None, final=final, tk=tk, sub=sub),
        grid=(query_tiles // step,),
        in_specs=[
            pl.BlockSpec((step, 1, HEAD_DIM, HEAD_DIM), lambda i: (i, 0, 0, 0)),
            pl.BlockSpec((HEAD_DIM, HEAD_DIM), lambda i: (0, 0)),
        ] + [pl.BlockSpec(memory_space=pl.ANY) for _ in pieces]
        + (state_specs if state is not None else []),
        out_specs=(pl.BlockSpec((step, HEAD_DIM, HEAD_DIM), lambda i: (i, 0, 0))
                   if final else state_specs),
        out_shape=(jax.ShapeDtypeStruct((query_tiles, HEAD_DIM, HEAD_DIM), BF16)
                   if final else state_shapes),
        scratch_shapes=[
            pltpu.VMEM((keys, HEAD_DIM, HEAD_DIM), BF16),
            pltpu.VMEM((keys, HEAD_DIM, HEAD_DIM), BF16),
            pltpu.VMEM((2, tk, tq), F32),
            pltpu.SemaphoreType.DMA((2 * len(pieces),)),
        ],
        compiler_params=pltpu.CompilerParams(vmem_limit_bytes=VMEM_BYTES),
        cost_estimate=pl.CostEstimate(
            flops=8 * query_tiles * keys * HEAD_DIM**3,
            transcendentals=query_tiles * keys * HEAD_DIM**2,
            bytes_accessed=4 * keys * HEAD_DIM**2,
        ),
        name=name,
    )(own, gate, *pieces, *(state or ()))
    return out


def post_kernel(a_ref, b_ref, c_ref, o_ref):
    def put(src, slot, head):
        o_ref[:, head * HEAD_DIM:(head + 1) * HEAD_DIM] = src[slot].astype(F32).T.astype(BF16)

    for slot in range(16):
        put(a_ref, slot, slot)
        put(b_ref, slot, 16 + slot)
    for slot in range(8):
        put(c_ref, slot, 32 + slot)


def collect(a, b, c):
    tokens = a.shape[2]
    width = HEAD_DIM * (2 * a.shape[0] + c.shape[0])
    return pl.pallas_call(
        post_kernel,
        out_shape=jax.ShapeDtypeStruct((tokens, width), BF16),
        compiler_params=pltpu.CompilerParams(vmem_limit_bytes=VMEM_BYTES),
        name="post",
    )(a, b, c)


def shift(axis, amount):
    size = lax.axis_size(axis)
    return [(i, (i + amount) % size) for i in range(size)]


def ring(pair, axis):
    half = pair.shape[0] // 2
    with jax.named_scope("near"):
        up = lax.ppermute(pair, axis, shift(axis, 1))
        down = lax.ppermute(pair, axis, shift(axis, -1))
    with jax.named_scope("far"):
        up_far = lax.ppermute(up[:half], axis, shift(axis, 1))
        down_far = lax.ppermute(down[half:], axis, shift(axis, -1))
    return [up, down, up_far, down_far]


def gates(timestep, gate_base, time_weight, first, count):
    half_freq = FREQ // 2
    exponent = jnp.arange(half_freq, dtype=jnp.int32).astype(F32) / half_freq
    frequency = jnp.power(F32(10000.0), -exponent)
    phase = timestep.astype(F32)[:, None] * frequency[None, :]
    embedded = jnp.concatenate([jnp.cos(phase), jnp.sin(phase)], axis=1)
    start = first * HEAD_DIM
    width = count * HEAD_DIM
    weight = lax.dynamic_slice_in_dim(time_weight, start, width, 1)
    base = lax.dynamic_slice_in_dim(gate_base, start, width, 0)
    projected = jnp.dot(embedded, weight, precision=lax.Precision.HIGHEST,
                        preferred_element_type=F32)
    gate = base + projected[0]
    return jnp.broadcast_to(gate.reshape(count, HEAD_DIM, 1), (count, HEAD_DIM, HEAD_DIM))


def local(queries, keys, values, query_gain, key_gain, timestep, gate_base, time_weight):
    x, z, y, core = (lax.axis_index(n) for n in ("x", "z", "y", "core"))
    block = (((x * 4 + z) * 4 + y) * 2 + core).reshape(1).astype(jnp.int32)
    by_z, by_y, by_z_only = ("x", "z", "core"), ("x", "y", "core"), ("x", "z")
    tensors = (block, queries, keys, values, query_gain, key_gain)
    spread = functools.partial(lax.all_to_all, split_axis=0, concat_axis=0, tiled=True)
    gate_of = functools.partial(gates, timestep, gate_base, time_weight)

    (a,) = prepare("prep_a", *tensors, ((0, 2),))
    b, c = prepare("prep_bc", *tensors, ((16, 2), (32, 1)))
    with jax.named_scope("spread_a"):
        a = spread(a, by_z)
    with jax.named_scope("ring_a"):
        up_a, down_a, up_far_a, down_far_a = ring(a[:, 1:], "y")
    b, a = lax.optimization_barrier((b, a))
    with jax.named_scope("spread_b"):
        b = spread(b, by_y)
    with jax.named_scope("ring_b"):
        up_b, down_b, up_far_b, down_far_b = ring(b[:, 1:], "z")
    c, b = lax.optimization_barrier((c, b))
    with jax.named_scope("spread_c"):
        c = spread(c, by_z_only)
    with jax.named_scope("ring_c"):
        pieces_c = [c[:, 1:]] + ring(c[:, 1:], "y")
    with jax.named_scope("pair_c"):
        pieces_c = pieces_c + [lax.ppermute(p, "core", shift("core", 1)) for p in pieces_c]
    gate_a = gate_of((x * 4 + z) * 2 + core, 1)[0]
    gate_b = gate_of(16 + (x * 4 + y) * 2 + core, 1)[0]
    gate_c = gate_of(32 + x * 4 + z, 1)[0]

    state = attend("attend_a1", a, gate_a, [a, up_a, down_a], final=False)
    out_a = attend("attend_a2", a, gate_a, [up_far_a, down_far_a], state)
    with jax.named_scope("return_a"):
        out_a = spread(out_a, by_z)
    state = attend("attend_b1", b, gate_b, [b, up_b, down_b], final=False)
    out_b = attend("attend_b2", b, gate_b, [up_far_b, down_far_b], state)
    with jax.named_scope("return_b"):
        out_b = spread(out_b, by_y)
    out_c = attend("attend_c", c, gate_c, pieces_c)
    with jax.named_scope("return_c"):
        out_c = spread(out_c, by_z_only)
    return collect(out_a, out_b, out_c)


def solution(mesh):
    fine = Mesh(mesh.devices.reshape(2, 2, 4, 4, 2), ("expert", "x", "z", "y", "core"))
    rows = P(("expert", "x", "z", "y", "core"), None)
    part = P("expert")
    return jax.shard_map(
        local,
        mesh=fine,
        in_specs=(rows, rows, rows, part, part, part, part, P("expert", None)),
        out_specs=rows,
        check_vma=False,
    )
```

```python
import functools
import math

import jax
import jax.numpy as jnp
import numpy as np
from jax import lax
from jax.experimental import pallas as pl
from jax.experimental.pallas import tpu as pltpu
from jax.sharding import Mesh
from jax.sharding import PartitionSpec as P


HEAD_DIM = 128
FREQ = 256
HGT = 32
WID = 32
EPSILON = 1e-06
LOG2E = 1.4426950408889634
SCALE = LOG2E / math.sqrt(HEAD_DIM)
VMEM_BYTES = 63 * 1024 * 1024
F32 = jnp.float32
BF16 = jnp.bfloat16


def inverse_row():
    half = HEAD_DIM // 2
    sixth = HEAD_DIM // 6
    frame = (HEAD_DIM - 4 * sixth) // 2
    j = np.arange(half)
    in_frame = j < frame
    in_row = (j >= frame) & (j < frame + sixth)
    local = np.where(in_frame, j, np.where(in_row, j - frame, j - frame - sixth))
    dims = np.where(in_frame, 2 * frame, 2 * sixth)
    inverse = np.power(10000.0, -2.0 * local / dims).astype(np.float32)
    kind = np.where(in_frame, 0, np.where(in_row, 1, 2))
    return np.repeat(inverse, 2), np.repeat(kind, 2)


def prep_kernel(block_ref, inv_hbm, *refs, tensors, plan):
    count = len(tensors)
    turned = [n for n, kind in enumerate(tensors) if kind != "v"]
    sources, refs = refs[:count], refs[count:]
    gains, refs = refs[:len(turned)], refs[len(turned):]
    outs, refs = refs[:len(plan)], refs[len(plan):]
    inv_ref, swap_ref, cos_ref, sin_ref, sems = refs[:5]
    bufs, refs = refs[5:5 + count], refs[5 + count:]
    gain_bufs, rms_refs = refs[:len(turned)], refs[len(turned):]
    tokens, width = bufs[0].shape
    step = pl.program_id(0)

    @pl.when(step == 0)
    def _():
        pairs = [(inv_hbm, inv_ref)] + list(zip(sources, bufs)) + list(zip(gains, gain_bufs))
        copies = [pltpu.make_async_copy(a, b, sems.at[n]) for n, (a, b) in enumerate(pairs)]
        for copy in copies:
            copy.start()
        lane = lax.broadcasted_iota(jnp.int32, (HEAD_DIM, HEAD_DIM), 1)
        depth = lax.broadcasted_iota(jnp.int32, (HEAD_DIM, HEAD_DIM), 0)
        below = jnp.where((lane % 2 == 0) & (depth == lane + 1), -1.0, 0.0)
        above = jnp.where((lane % 2 == 1) & (depth == lane - 1), 1.0, 0.0)
        swap_ref[...] = (below + above).astype(BF16)
        copies[0].wait()
        token = block_ref[0] * tokens + lax.broadcasted_iota(jnp.int32, (tokens, HEAD_DIM), 0)
        pair = lax.broadcasted_iota(jnp.int32, (tokens, HEAD_DIM), 1) // 2
        sixth = HEAD_DIM // 6
        frame_pairs = (HEAD_DIM - 4 * sixth) // 2
        frame = token // (HGT * WID)
        row = (token // WID) % HGT
        column = token % WID
        coord = jnp.where(pair < frame_pairs, frame,
                          jnp.where(pair < frame_pairs + sixth, row, column)).astype(F32)
        angle = coord * inv_ref[...]
        cos_ref[...] = jnp.cos(angle)
        sin_ref[...] = jnp.sin(angle)
        for copy in copies[1:]:
            copy.wait()
        for src, dst in zip([bufs[n] for n in turned], rms_refs):
            total = jnp.zeros((tokens, HEAD_DIM), F32)
            for h in range(width // HEAD_DIM):
                x = src[:, h * HEAD_DIM:(h + 1) * HEAD_DIM].astype(F32)
                total = total + x * x
            mean = jnp.sum(total, axis=1, keepdims=True) / width
            dst[...] = jnp.broadcast_to(lax.rsqrt(mean + EPSILON), (tokens, HEAD_DIM))

    even = lax.broadcasted_iota(jnp.int32, (1, HEAD_DIM), 1) % 2 == 0

    def columns(n, head):
        return bufs[n][:, pl.ds(pl.multiple_of(head * HEAD_DIM, HEAD_DIM), HEAD_DIM)]

    def rotated(n, head):
        x = columns(n, head)
        xs = jnp.dot(x, swap_ref[...], preferred_element_type=F32)
        g = gain_bufs[turned.index(n)][pl.ds(head, 1), :]
        gs = jnp.where(even, pltpu.roll(g, HEAD_DIM - 1, 1), pltpu.roll(g, 1, 1))
        r = rms_refs[turned.index(n)][...]
        return (x.astype(F32) * r * g) * cos_ref[...] + (xs * r * gs) * sin_ref[...]

    for dst, (first, peers, heads, kinds) in zip(outs, plan):
        for peer in range(peers):
            for h in range(heads):
                head = first + (step * peers + peer) * heads + h
                for slot, kind in enumerate(kinds):
                    n = tensors.index(kind)
                    y = columns(n, head).astype(F32) if kind == "v" else rotated(n, head)
                    dst[peer, h, slot] = (y if kind == "k" else y.T).astype(BF16)


def prepare(steps, block, tensors, plan):
    kinds = tuple(tensors)
    tokens, width = tensors[kinds[0]][0].shape
    heads = width // HEAD_DIM
    inverse, _ = inverse_row()
    tile = (HEAD_DIM, tokens)
    gains = [tensors[k][1].reshape(heads, HEAD_DIM) for k in kinds if k != "v"]
    hbm = pl.BlockSpec(memory_space=pltpu.HBM)
    shapes = [(peers, count, len(slots)) + tile for _, peers, count, slots in plan]
    return pl.pallas_call(
        functools.partial(prep_kernel, tensors=kinds, plan=plan),
        grid=(steps,),
        in_specs=[pl.BlockSpec(memory_space=pltpu.SMEM)] + [hbm] * (1 + len(kinds) + len(gains)),
        out_specs=[pl.BlockSpec(shape, lambda i: (i, 0, 0, 0, 0)) for shape in shapes],
        out_shape=[jax.ShapeDtypeStruct((steps * shape[0],) + shape[1:], BF16)
                   for shape in shapes],
        scratch_shapes=[
            pltpu.VMEM((1, HEAD_DIM), F32),
            pltpu.VMEM((HEAD_DIM, HEAD_DIM), BF16),
            pltpu.VMEM((tokens, HEAD_DIM), F32),
            pltpu.VMEM((tokens, HEAD_DIM), F32),
            pltpu.SemaphoreType.DMA((1 + len(kinds) + len(gains),)),
        ] + [pltpu.VMEM((tokens, width), BF16) for _ in kinds]
        + [pltpu.VMEM((heads, HEAD_DIM), F32) for _ in gains]
        + [pltpu.VMEM((tokens, HEAD_DIM), F32) for _ in gains],
        compiler_params=pltpu.CompilerParams(vmem_limit_bytes=VMEM_BYTES),
    )(block, jnp.asarray(inverse)[None, :], *[tensors[k][0] for k in kinds], *gains)


def attend_kernel(*refs, sizes, shifts, resume, final, tk, sub):
    count = len(sizes)
    q_ref, gate_ref = refs[:2]
    pieces = refs[2:2 + count]
    at = 2 + count
    if resume:
        stat_in, mixed_in = refs[at:at + 2]
        at += 2
    if final:
        o_ref = refs[at]
        at += 1
    else:
        stat_out, mixed_out = refs[at:at + 2]
        at += 2
    k_bufs, v_bufs, s_buf, sems = refs[at:]
    head = pl.program_id(0)
    slot = head % 2

    def loads(head, slot):
        copies = []
        offset = 0
        for i, size in enumerate(sizes):
            for j, buf in enumerate((k_bufs, v_bufs)):
                copies.append(pltpu.make_async_copy(
                    pieces[i].at[:, head, shifts[i] + j], buf.at[slot, pl.ds(offset, size)],
                    sems.at[slot, 2 * i + j]))
            offset += size
        return copies

    @pl.when(pl.program_id(1) == 0)
    def _():
        @pl.when(head == 0)
        def _():
            for copy in loads(head, slot):
                copy.start()

        @pl.when(head + 1 < pl.num_programs(0))
        def _():
            for copy in loads(head + 1, 1 - slot):
                copy.start()

        for copy in loads(head, slot):
            copy.wait()

    k_buf, v_buf = k_bufs.at[slot], v_bufs.at[slot]
    tiles = q_ref.shape[0]
    tq = tiles * HEAD_DIM
    q = jnp.concatenate([q_ref[t, 0, 0] for t in range(tiles)], axis=1).astype(F32) * SCALE
    q_high = q.astype(BF16)
    q_low = (q - q_high.astype(F32)).astype(BF16)
    q_both = jnp.concatenate([q_high, q_low], axis=0)
    blocks = sum(sizes) * HEAD_DIM // tk
    subs = tk // sub
    per_sub = sub // HEAD_DIM

    def scores(j, i):
        first = (j * subs + i) * per_sub
        k = k_buf[first:first + per_sub].reshape(sub, HEAD_DIM)
        s = jnp.dot(jnp.concatenate([k, k], axis=1), q_both, preferred_element_type=F32)
        s_buf[j % 2, i * sub:(i + 1) * sub, :] = s
        return jnp.max(s.reshape(sub // 8, 8, tq), axis=0)

    top = scores(0, 0)
    for i in range(1, subs):
        top = jnp.maximum(top, scores(0, i))
    if resume:
        peak = stat_in[0, 0:1, :]
        total = stat_in[0, 8:16, :]
        mixed = mixed_in[0]
    else:
        peak = jnp.full((1, tq), -1e30, F32)
        total = jnp.zeros((8, tq), F32)
        mixed = jnp.zeros((HEAD_DIM, tq), F32)
    for j in range(blocks):
        new_peak = jnp.maximum(peak, jnp.max(top, axis=0, keepdims=True))
        shrink = jnp.exp2(peak - new_peak)
        total = total * shrink
        part = None
        top = None
        for i in range(subs):
            if j + 1 < blocks:
                t = scores(j + 1, i)
                top = t if top is None else jnp.maximum(top, t)
            e = jnp.exp2(s_buf[j % 2, i * sub:(i + 1) * sub, :] - new_peak)
            total = total + jnp.sum(e.reshape(sub // 8, 8, tq), axis=0)
            first = (j * subs + i) * per_sub
            v = jnp.concatenate([v_buf[first + t] for t in range(per_sub)], axis=1)
            d = jnp.dot(v, e.astype(BF16), preferred_element_type=F32)
            part = d if part is None else part + d
        mixed = mixed * shrink + part
        peak = new_peak
    if final:
        out = mixed / jnp.sum(total, axis=0, keepdims=True)
        gate = gate_ref[0]
        for t in range(tiles):
            o_ref[t, 0] = (out[:, t * HEAD_DIM:(t + 1) * HEAD_DIM] * gate).astype(BF16)
    else:
        stat_out[0, 0:8, :] = jnp.broadcast_to(peak, (8, tq))
        stat_out[0, 8:16, :] = total
        mixed_out[0] = mixed


def attend(query, gate, pieces, state=None, final=True, tq=512, tk=1024, sub=1024):
    sizes = tuple(p.shape[0] for p in pieces)
    shifts = tuple(p.shape[2] - 2 for p in pieces)
    query_tiles, heads = query.shape[:2]
    step = tq // HEAD_DIM
    keys = sum(sizes)
    slots = min(heads, 2)
    state_specs = [pl.BlockSpec((1, 16, tq), lambda h, i: (h, 0, i)),
                   pl.BlockSpec((1, HEAD_DIM, tq), lambda h, i: (h, 0, i))]
    state_shapes = [jax.ShapeDtypeStruct((heads, 16, query_tiles * HEAD_DIM), F32),
                    jax.ShapeDtypeStruct((heads, HEAD_DIM, query_tiles * HEAD_DIM), F32)]
    return pl.pallas_call(
        functools.partial(attend_kernel, sizes=sizes, shifts=shifts,
                          resume=state is not None, final=final, tk=tk, sub=sub),
        grid=(heads, query_tiles // step),
        in_specs=[
            pl.BlockSpec((step, 1, 1, HEAD_DIM, HEAD_DIM), lambda h, i: (i, h, 0, 0, 0)),
            pl.BlockSpec((1, HEAD_DIM, HEAD_DIM), lambda h, i: (h, 0, 0)),
        ] + [pl.BlockSpec(memory_space=pl.ANY) for _ in pieces]
        + (state_specs if state is not None else []),
        out_specs=(pl.BlockSpec((step, 1, HEAD_DIM, HEAD_DIM), lambda h, i: (i, h, 0, 0))
                   if final else state_specs),
        out_shape=(jax.ShapeDtypeStruct((query_tiles, heads, HEAD_DIM, HEAD_DIM), BF16)
                   if final else state_shapes),
        scratch_shapes=[
            pltpu.VMEM((slots, keys, HEAD_DIM, HEAD_DIM), BF16),
            pltpu.VMEM((slots, keys, HEAD_DIM, HEAD_DIM), BF16),
            pltpu.VMEM((2, tk, tq), F32),
            pltpu.SemaphoreType.DMA((slots, 2 * len(pieces))),
        ],
        compiler_params=pltpu.CompilerParams(vmem_limit_bytes=VMEM_BYTES),
        cost_estimate=pl.CostEstimate(
            flops=8 * heads * query_tiles * keys * HEAD_DIM**3,
            transcendentals=heads * query_tiles * keys * HEAD_DIM**2,
            bytes_accessed=4 * heads * keys * HEAD_DIM**2,
        ),
    )(query, gate, *pieces, *(state or ()))


def post_kernel(*refs):
    o_ref = refs[-1]
    head = 0
    for src in refs[:-1]:
        for peer in range(src.shape[0]):
            for h in range(src.shape[1]):
                tile = src[peer, h].astype(F32).T.astype(BF16)
                o_ref[:, head * HEAD_DIM:(head + 1) * HEAD_DIM] = tile
                head += 1


def collect(*parts):
    tokens = parts[0].shape[-1]
    width = HEAD_DIM * sum(p.shape[0] * p.shape[1] for p in parts)
    return pl.pallas_call(
        post_kernel,
        out_shape=jax.ShapeDtypeStruct((tokens, width), BF16),
        compiler_params=pltpu.CompilerParams(vmem_limit_bytes=VMEM_BYTES),
        name="post",
    )(*parts)


def shift(axis, amount):
    size = lax.axis_size(axis)
    return [(i, (i + amount) % size) for i in range(size)]


def ring(pair, axis):
    half = pair.shape[0] // 2
    up = lax.ppermute(pair, axis, shift(axis, 1))
    down = lax.ppermute(pair, axis, shift(axis, -1))
    up_far = lax.ppermute(up[:half], axis, shift(axis, 1))
    down_far = lax.ppermute(down[half:], axis, shift(axis, -1))
    return [up, down, up_far, down_far]


def gates(timestep, gate_base, time_weight, first, count):
    half_freq = FREQ // 2
    exponent = jnp.arange(half_freq, dtype=jnp.int32).astype(F32) / half_freq
    frequency = jnp.power(F32(10000.0), -exponent)
    phase = timestep.astype(F32)[:, None] * frequency[None, :]
    embedded = jnp.concatenate([jnp.cos(phase), jnp.sin(phase)], axis=1)
    start = first * HEAD_DIM
    width = count * HEAD_DIM
    weight = lax.dynamic_slice_in_dim(time_weight, start, width, 1)
    base = lax.dynamic_slice_in_dim(gate_base, start, width, 0)
    projected = jnp.dot(embedded, weight, precision=lax.Precision.HIGHEST,
                        preferred_element_type=F32)
    gate = base + projected[0]
    return jnp.broadcast_to(gate.reshape(count, HEAD_DIM, 1), (count, HEAD_DIM, HEAD_DIM))


def block_attention(queries, keys, values, query_gain, key_gain, timestep, gate_base, time_weight):
    x, z, y, core = (lax.axis_index(n) for n in ("x", "z", "y", "core"))
    block = (((x * 4 + z) * 4 + y) * 2 + core).reshape(1).astype(jnp.int32)
    wide, narrow = ("x", "z", "core"), ("x", "z")
    spread = functools.partial(lax.all_to_all, split_axis=0, concat_axis=0, tiled=True)
    gate_of = functools.partial(gates, timestep, gate_base, time_weight)
    q, k, v = (queries, query_gain), (keys, key_gain), (values, None)

    (a,) = prepare(4, block, {"k": k, "v": v}, ((0, 4, 1, "kv"),))
    a_query, b = prepare(8, block, {"q": q, "k": k, "v": v},
                         ((0, 2, 1, "q"), (16, 1, 3, "qkv")))
    a = spread(a, wide)
    ring_a = ring(a, "y")
    b, a = lax.optimization_barrier((b, a))
    b = spread(b, narrow)
    own_b = b[:, :, 1:]
    ring_b = ring(own_b, "y")
    a_query, b = lax.optimization_barrier((a_query, b))
    a_query = spread(a_query, wide)
    near_b = [own_b] + ring_b[:2]
    near_b = near_b + [lax.ppermute(p, "core", shift("core", 1)) for p in near_b]
    far_b = ring_b[2:] + [lax.ppermute(p, "core", shift("core", 1)) for p in ring_b[2:]]
    gate_a = gate_of((x * 4 + z) * 2 + core, 1)
    gate_b = gate_of(16 + (x * 4 + z) * 3, 3)

    out_a = attend(a_query, gate_a, [a] + ring_a)
    out_a = spread(out_a, wide)
    state = attend(b, gate_b, near_b, final=False)
    out_b = attend(b, gate_b, far_b, state)
    out_b = spread(out_b, narrow)
    return collect(out_a, out_b)


def solution(mesh):
    fine = Mesh(mesh.devices.reshape(2, 2, 4, 4, 2), ("expert", "x", "z", "y", "core"))
    rows = P(("expert", "x", "z", "y", "core"), None)
    part = P("expert")
    return jax.shard_map(
        block_attention,
        mesh=fine,
        in_specs=(rows, rows, rows, part, part, part, part, P("expert", None)),
        out_specs=rows,
        check_vma=False,
    )
```

```python
import functools
import math

import jax
import jax.numpy as jnp
import numpy as np
from jax import lax
from jax.experimental import pallas as pl
from jax.experimental.pallas import tpu as pltpu
from jax.sharding import Mesh
from jax.sharding import PartitionSpec as P


HEAD_DIM = 128
FREQ = 256
HGT = 32
WID = 32
EPSILON = 1e-06
LOG2E = 1.4426950408889634
SMALLEST = 2.0**-80
LARGEST = 2.0**100
SCALE = LOG2E / math.sqrt(HEAD_DIM)
VMEM_BYTES = 63 * 1024 * 1024
F32 = jnp.float32
BF16 = jnp.bfloat16


def inverse_row():
    half = HEAD_DIM // 2
    sixth = HEAD_DIM // 6
    frame = (HEAD_DIM - 4 * sixth) // 2
    j = np.arange(half)
    in_frame = j < frame
    in_row = (j >= frame) & (j < frame + sixth)
    local = np.where(in_frame, j, np.where(in_row, j - frame, j - frame - sixth))
    dims = np.where(in_frame, 2 * frame, 2 * sixth)
    inverse = np.power(10000.0, -2.0 * local / dims).astype(np.float32)
    kind = np.where(in_frame, 0, np.where(in_row, 1, 2))
    return np.repeat(inverse, 2), np.repeat(kind, 2)


def prep_kernel(block_ref, inv_hbm, *refs, tensors, plan):
    count = len(tensors)
    turned = [n for n, kind in enumerate(tensors) if kind != "v"]
    sources, refs = refs[:count], refs[count:]
    gains, refs = refs[:len(turned)], refs[len(turned):]
    outs, refs = refs[:len(plan)], refs[len(plan):]
    inv_ref, swap_ref, cos_ref, sin_ref, sems = refs[:5]
    bufs, refs = refs[5:5 + count], refs[5 + count:]
    gain_bufs, rms_refs = refs[:len(turned)], refs[len(turned):]
    tokens, width = bufs[0].shape
    step = pl.program_id(0)

    @pl.when(step == 0)
    def _():
        pairs = [(inv_hbm, inv_ref)] + list(zip(sources, bufs)) + list(zip(gains, gain_bufs))
        copies = [pltpu.make_async_copy(a, b, sems.at[n]) for n, (a, b) in enumerate(pairs)]
        for copy in copies:
            copy.start()
        lane = lax.broadcasted_iota(jnp.int32, (HEAD_DIM, HEAD_DIM), 1)
        depth = lax.broadcasted_iota(jnp.int32, (HEAD_DIM, HEAD_DIM), 0)
        below = jnp.where((lane % 2 == 0) & (depth == lane + 1), -1.0, 0.0)
        above = jnp.where((lane % 2 == 1) & (depth == lane - 1), 1.0, 0.0)
        swap_ref[...] = (below + above).astype(BF16)
        copies[0].wait()
        token = block_ref[0] * tokens + lax.broadcasted_iota(jnp.int32, (tokens, HEAD_DIM), 0)
        pair = lax.broadcasted_iota(jnp.int32, (tokens, HEAD_DIM), 1) // 2
        sixth = HEAD_DIM // 6
        frame_pairs = (HEAD_DIM - 4 * sixth) // 2
        frame = token // (HGT * WID)
        row = (token // WID) % HGT
        column = token % WID
        coord = jnp.where(pair < frame_pairs, frame,
                          jnp.where(pair < frame_pairs + sixth, row, column)).astype(F32)
        angle = coord * inv_ref[...]
        cos_ref[...] = jnp.cos(angle)
        sin_ref[...] = jnp.sin(angle)
        for copy in copies[1:]:
            copy.wait()
        for src, dst in zip([bufs[n] for n in turned], rms_refs):
            total = jnp.zeros((tokens, HEAD_DIM), F32)
            for h in range(width // HEAD_DIM):
                x = src[:, h * HEAD_DIM:(h + 1) * HEAD_DIM].astype(F32)
                total = total + x * x
            mean = jnp.sum(total, axis=1, keepdims=True) / width
            dst[...] = jnp.broadcast_to(lax.rsqrt(mean + EPSILON), (tokens, HEAD_DIM))

    even = lax.broadcasted_iota(jnp.int32, (1, HEAD_DIM), 1) % 2 == 0

    def columns(n, head):
        return bufs[n][:, pl.ds(pl.multiple_of(head * HEAD_DIM, HEAD_DIM), HEAD_DIM)]

    def rotated(n, head):
        x = columns(n, head)
        xs = jnp.dot(x, swap_ref[...], preferred_element_type=F32)
        g = gain_bufs[turned.index(n)][pl.ds(head, 1), :]
        gs = jnp.where(even, pltpu.roll(g, HEAD_DIM - 1, 1), pltpu.roll(g, 1, 1))
        r = rms_refs[turned.index(n)][...]
        return (x.astype(F32) * r * g) * cos_ref[...] + (xs * r * gs) * sin_ref[...]

    for dst, (first, peers, heads, kinds) in zip(outs, plan):
        for peer in range(peers):
            for h in range(heads):
                head = first + (step * peers + peer) * heads + h
                for slot, kind in enumerate(kinds):
                    n = tensors.index(kind)
                    y = columns(n, head).astype(F32) if kind == "v" else rotated(n, head)
                    dst[peer, h, slot] = (y if kind == "k" else y.T).astype(BF16)


def prepare(steps, block, tensors, plan):
    kinds = tuple(tensors)
    tokens, width = tensors[kinds[0]][0].shape
    heads = width // HEAD_DIM
    inverse, _ = inverse_row()
    tile = (HEAD_DIM, tokens)
    gains = [tensors[k][1].reshape(heads, HEAD_DIM) for k in kinds if k != "v"]
    hbm = pl.BlockSpec(memory_space=pltpu.HBM)
    shapes = [(peers, count, len(slots)) + tile for _, peers, count, slots in plan]
    return pl.pallas_call(
        functools.partial(prep_kernel, tensors=kinds, plan=plan),
        grid=(steps,),
        in_specs=[pl.BlockSpec(memory_space=pltpu.SMEM)] + [hbm] * (1 + len(kinds) + len(gains)),
        out_specs=[pl.BlockSpec(shape, lambda i: (i, 0, 0, 0, 0)) for shape in shapes],
        out_shape=[jax.ShapeDtypeStruct((steps * shape[0],) + shape[1:], BF16)
                   for shape in shapes],
        scratch_shapes=[
            pltpu.VMEM((1, HEAD_DIM), F32),
            pltpu.VMEM((HEAD_DIM, HEAD_DIM), BF16),
            pltpu.VMEM((tokens, HEAD_DIM), F32),
            pltpu.VMEM((tokens, HEAD_DIM), F32),
            pltpu.SemaphoreType.DMA((1 + len(kinds) + len(gains),)),
        ] + [pltpu.VMEM((tokens, width), BF16) for _ in kinds]
        + [pltpu.VMEM((heads, HEAD_DIM), F32) for _ in gains]
        + [pltpu.VMEM((tokens, HEAD_DIM), F32) for _ in gains],
        compiler_params=pltpu.CompilerParams(vmem_limit_bytes=VMEM_BYTES),
    )(block, jnp.asarray(inverse)[None, :], *[tensors[k][0] for k in kinds], *gains)


def attend_kernel(*refs, sizes, resume, final, sub, together):
    count = len(sizes)
    q_ref, gate_ref = refs[:2]
    pieces = refs[2:2 + count]
    at = 2 + count
    if resume:
        stat_in, mixed_in = refs[at:at + 2]
        at += 2
    if final:
        o_ref = refs[at]
        at += 1
    else:
        stat_out, mixed_out = refs[at:at + 2]
        at += 2
    k_bufs, v_bufs, sems = refs[at:]
    group = pl.program_id(0)
    base = (group % 2) * together

    def loads(group, base):
        copies = []
        for h in range(together):
            offset = 0
            for i, size in enumerate(sizes):
                for j, buf in enumerate((k_bufs, v_bufs)):
                    copies.append(pltpu.make_async_copy(
                        pieces[i].at[:, group * together + h, j],
                        buf.at[base + h, pl.ds(offset, size)],
                        sems.at[base + h, 2 * i + j]))
                offset += size
        return copies

    @pl.when(pl.program_id(1) == 0)
    def _():
        @pl.when(group == 0)
        def _():
            for copy in loads(group, base):
                copy.start()

        @pl.when(group + 1 < pl.num_programs(0))
        def _():
            for copy in loads(group + 1, together - base):
                copy.start()

        for copy in loads(group, base):
            copy.wait()

    tiles = q_ref.shape[0]
    tq = tiles * HEAD_DIM
    key_tiles = sum(sizes)
    per_sub = sub // HEAD_DIM
    subs = key_tiles // per_sub

    def scaled(q):
        q = q.astype(F32) * SCALE
        high = q.astype(BF16)
        low = (q - high.astype(F32)).astype(BF16)
        return jnp.concatenate([high, low], axis=0)

    def scores(h, first, count, q_both):
        k = k_bufs[base + h, pl.ds(first, count)].reshape(count * HEAD_DIM, HEAD_DIM)
        return jnp.dot(jnp.concatenate([k, k], axis=1), q_both, preferred_element_type=F32)

    def weighted(h, first, count, e):
        v = jnp.concatenate([v_bufs[base + h, first + t] for t in range(count)], axis=1)
        return jnp.dot(v, e.astype(BF16), preferred_element_type=F32)

    def emit(h, tile, out):
        o_ref[tile, h] = (out * gate_ref[h]).astype(BF16)

    queries = [scaled(jnp.concatenate([q_ref[t, h, 0] for t in range(tiles)], axis=1))
               for h in range(together)]
    items = [(h, j) for h in range(together) for j in range(subs)]
    safe = None
    s = scores(0, 0, per_sub, queries[0])
    for n, (h, j) in enumerate(items):
        after = None
        if n + 1 < len(items):
            nh, nj = items[n + 1]
            after = scores(nh, nj * per_sub, per_sub, queries[nh])
        if j == 0:
            total = jnp.zeros((8, tq), F32)
            mixed = None
        e = jnp.exp2(s)
        total = total + jnp.sum(e.reshape(sub // 8, 8, tq), axis=0)
        d = weighted(h, j * per_sub, per_sub, e)
        mixed = d if mixed is None else mixed + d
        s = after
        if j + 1 < subs:
            continue
        if resume:
            total = total + stat_in[h, 8:16, :]
            mixed = mixed + mixed_in[h]
        row = jnp.sum(total, axis=0, keepdims=True)
        fine = (row > SMALLEST) & (row < LARGEST)
        if resume:
            fine = fine & (stat_in[h, 0:1, :] == 0.0)
        fine = jnp.where(fine, 1.0, 0.0)
        safe = fine if safe is None else jnp.minimum(safe, fine)
        if final:
            out = mixed / row
            for t in range(tiles):
                emit(h, t, out[:, t * HEAD_DIM:(t + 1) * HEAD_DIM])
        else:
            stat_out[h, 0:8, :] = jnp.zeros((8, tq), F32)
            stat_out[h, 8:16, :] = total
            mixed_out[h] = mixed

    @pl.when(jnp.min(safe) < 0.5)
    def _():
        def one_tile(n, carry):
            h = n // tiles
            t = n % tiles
            q_tile = scaled(q_ref[t, h, 0])
            lanes = pl.ds(pl.multiple_of(t * HEAD_DIM, HEAD_DIM), HEAD_DIM)
            if resume:
                state = (stat_in[h, 0:1, lanes], stat_in[h, 8:16, lanes], mixed_in[h, :, lanes])
            else:
                state = (jnp.full((1, HEAD_DIM), -1e30, F32), jnp.zeros((8, HEAD_DIM), F32),
                         jnp.zeros((HEAD_DIM, HEAD_DIM), F32))

            def one_block(j, state):
                peak, total, mixed = state
                s = scores(h, j * 8, 8, q_tile)
                new_peak = jnp.maximum(peak, jnp.max(s, axis=0, keepdims=True))
                shrink = jnp.exp2(peak - new_peak)
                e = jnp.exp2(s - new_peak)
                total = total * shrink + jnp.sum(e.reshape(HEAD_DIM, 8, HEAD_DIM), axis=0)
                return new_peak, total, mixed * shrink + weighted(h, j * 8, 8, e)

            peak, total, mixed = lax.fori_loop(0, key_tiles // 8, one_block, state)
            if final:
                emit(h, t, mixed / jnp.sum(total, axis=0, keepdims=True))
            else:
                stat_out[h, 0:8, lanes] = jnp.broadcast_to(peak, (8, HEAD_DIM))
                stat_out[h, 8:16, lanes] = total
                mixed_out[h, :, lanes] = mixed
            return carry

        lax.fori_loop(0, together * tiles, one_tile, 0)


def attend(query, gate, pieces, state=None, final=True, tq=1024, sub=512, together=1):
    sizes = tuple(p.shape[0] for p in pieces)
    query_tiles, heads = query.shape[:2]
    step = tq // HEAD_DIM
    keys = sum(sizes)
    slots = together * min(heads // together, 2)
    state_specs = [pl.BlockSpec((together, 16, tq), lambda h, i: (h, 0, i)),
                   pl.BlockSpec((together, HEAD_DIM, tq), lambda h, i: (h, 0, i))]
    state_shapes = [jax.ShapeDtypeStruct((heads, 16, query_tiles * HEAD_DIM), F32),
                    jax.ShapeDtypeStruct((heads, HEAD_DIM, query_tiles * HEAD_DIM), F32)]
    return pl.pallas_call(
        functools.partial(attend_kernel, sizes=sizes, resume=state is not None, final=final,
                          sub=sub, together=together),
        grid=(heads // together, query_tiles // step),
        in_specs=[
            pl.BlockSpec((step, together, 1, HEAD_DIM, HEAD_DIM), lambda h, i: (i, h, 0, 0, 0)),
            pl.BlockSpec((together, HEAD_DIM, HEAD_DIM), lambda h, i: (h, 0, 0)),
        ] + [pl.BlockSpec(memory_space=pl.ANY) for _ in pieces]
        + (state_specs if state is not None else []),
        out_specs=(pl.BlockSpec((step, together, HEAD_DIM, HEAD_DIM), lambda h, i: (i, h, 0, 0))
                   if final else state_specs),
        out_shape=(jax.ShapeDtypeStruct((query_tiles, heads, HEAD_DIM, HEAD_DIM), BF16)
                   if final else state_shapes),
        scratch_shapes=[
            pltpu.VMEM((slots, keys, HEAD_DIM, HEAD_DIM), BF16),
            pltpu.VMEM((slots, keys, HEAD_DIM, HEAD_DIM), BF16),
            pltpu.SemaphoreType.DMA((slots, 2 * len(pieces))),
        ],
        compiler_params=pltpu.CompilerParams(vmem_limit_bytes=VMEM_BYTES),
        cost_estimate=pl.CostEstimate(
            flops=8 * heads * query_tiles * keys * HEAD_DIM**3,
            transcendentals=heads * query_tiles * keys * HEAD_DIM**2,
            bytes_accessed=4 * heads * keys * HEAD_DIM**2,
        ),
    )(query, gate, *pieces, *(state or ()))


def post_kernel(*refs):
    o_ref = refs[-1]
    head = 0
    for src in refs[:-1]:
        for peer in range(src.shape[0]):
            for h in range(src.shape[1]):
                tile = src[peer, h].astype(F32).T.astype(BF16)
                o_ref[:, head * HEAD_DIM:(head + 1) * HEAD_DIM] = tile
                head += 1


def collect(*parts):
    tokens = parts[0].shape[-1]
    width = HEAD_DIM * sum(p.shape[0] * p.shape[1] for p in parts)
    return pl.pallas_call(
        post_kernel,
        out_shape=jax.ShapeDtypeStruct((tokens, width), BF16),
        compiler_params=pltpu.CompilerParams(vmem_limit_bytes=16 * 1024 * 1024),
        name="post",
    )(*parts)


def shift(axis, amount):
    size = lax.axis_size(axis)
    return [(i, (i + amount) % size) for i in range(size)]


def ring(low, high, axis):
    up_low = lax.ppermute(low, axis, shift(axis, 1))
    down_high = lax.ppermute(high, axis, shift(axis, -1))
    up_high = lax.ppermute(high, axis, shift(axis, 1))
    down_low = lax.ppermute(low, axis, shift(axis, -1))
    up_far = lax.ppermute(up_low, axis, shift(axis, 1))
    down_far = lax.ppermute(down_high, axis, shift(axis, -1))
    return [up_low, down_high, up_high, down_low], [up_far, down_far]


def gates(timestep, gate_base, time_weight, first, count):
    half_freq = FREQ // 2
    exponent = jnp.arange(half_freq, dtype=jnp.int32).astype(F32) / half_freq
    frequency = jnp.power(F32(10000.0), -exponent)
    phase = timestep.astype(F32)[:, None] * frequency[None, :]
    embedded = jnp.concatenate([jnp.cos(phase), jnp.sin(phase)], axis=1)
    start = first * HEAD_DIM
    width = count * HEAD_DIM
    weight = lax.dynamic_slice_in_dim(time_weight, start, width, 1)
    base = lax.dynamic_slice_in_dim(gate_base, start, width, 0)
    projected = jnp.dot(embedded, weight, precision=lax.Precision.HIGHEST,
                        preferred_element_type=F32)
    gate = base + projected[0]
    return jnp.broadcast_to(gate.reshape(count, HEAD_DIM, 1), (count, HEAD_DIM, HEAD_DIM))


def block_attention(queries, keys, values, query_gain, key_gain, timestep, gate_base, time_weight):
    x, z, y, core = (lax.axis_index(n) for n in ("x", "z", "y", "core"))
    block = (((x * 4 + z) * 4 + y) * 2 + core).reshape(1).astype(jnp.int32)
    wide, narrow = ("x", "z", "core"), ("x", "z")
    spread = functools.partial(lax.all_to_all, split_axis=0, concat_axis=0, tiled=True)
    gate_of = functools.partial(gates, timestep, gate_base, time_weight)
    q, k, v = (queries, query_gain), (keys, key_gain), (values, None)

    (a,) = prepare(4, block, {"k": k, "v": v}, ((0, 4, 1, "kv"),))
    b, a_query, b_query = prepare(8, block, {"q": q, "k": k, "v": v},
                                  ((16, 1, 3, "kv"), (0, 2, 1, "q"), (16, 1, 3, "q")))
    a = spread(a, wide)
    up_a = lax.ppermute(a, "y", shift("y", 1))
    down_a = lax.ppermute(a, "y", shift("y", -1))
    far_a = [lax.ppermute(up_a[:8], "y", shift("y", 1)),
             lax.ppermute(down_a[8:], "y", shift("y", -1))]
    b, a = lax.optimization_barrier((b, a))
    b = spread(b, narrow)
    own_b = [b[:4], b[4:]]
    near_b, far_b = ring(*own_b, "y")
    a_query, b = lax.optimization_barrier((a_query, b))
    a_query = spread(a_query, wide)
    b_query, a_query = lax.optimization_barrier((b_query, a_query))
    b_query = spread(b_query, narrow)

    def other(parts):
        return [lax.ppermute(p, "core", shift("core", 1)) for p in parts]

    near_b = [b] + near_b + other(own_b) + other(near_b)
    far_b = far_b + other(far_b)
    gate_a = gate_of((x * 4 + z) * 2 + core, 1)
    gate_b = gate_of(16 + (x * 4 + z) * 3, 3)

    out_a = attend(a_query, gate_a, [a, up_a, down_a] + far_a)
    out_a = spread(out_a, wide)
    state = attend(b_query, gate_b, near_b, final=False)
    out_b = attend(b_query, gate_b, far_b, state, together=3)
    out_b = spread(out_b, narrow)
    return collect(out_a, out_b)


def solution(mesh):
    fine = Mesh(mesh.devices.reshape(2, 2, 4, 4, 2), ("expert", "x", "z", "y", "core"))
    rows = P(("expert", "x", "z", "y", "core"), None)
    part = P("expert")
    return jax.shard_map(
        block_attention,
        mesh=fine,
        in_specs=(rows, rows, rows, part, part, part, part, P("expert", None)),
        out_specs=rows,
        check_vma=False,
    )
```

```python
import functools
import math

import jax
import jax.numpy as jnp
import numpy as np
from jax import lax
from jax.experimental import pallas as pl
from jax.experimental.pallas import tpu as pltpu
from jax.sharding import Mesh
from jax.sharding import PartitionSpec as P


HEAD_DIM = 128
FREQ = 256
HGT = 32
WID = 32
EPSILON = 1e-06
LOG2E = 1.4426950408889634
SMALLEST = 2.0**-80
LARGEST = 2.0**100
SCALE = LOG2E / math.sqrt(HEAD_DIM)
VMEM_BYTES = 63 * 1024 * 1024
F32 = jnp.float32
BF16 = jnp.bfloat16


def inverse_row():
    half = HEAD_DIM // 2
    sixth = HEAD_DIM // 6
    frame = (HEAD_DIM - 4 * sixth) // 2
    j = np.arange(half)
    in_frame = j < frame
    in_row = (j >= frame) & (j < frame + sixth)
    local = np.where(in_frame, j, np.where(in_row, j - frame, j - frame - sixth))
    dims = np.where(in_frame, 2 * frame, 2 * sixth)
    inverse = np.power(10000.0, -2.0 * local / dims).astype(np.float32)
    kind = np.where(in_frame, 0, np.where(in_row, 1, 2))
    return np.repeat(inverse, 2), np.repeat(kind, 2)


def prep_kernel(block_ref, inv_hbm, *refs, tensors, plan):
    count = len(tensors)
    turned = [n for n, kind in enumerate(tensors) if kind != "v"]
    sources, refs = refs[:count], refs[count:]
    gains, refs = refs[:len(turned)], refs[len(turned):]
    outs, refs = refs[:len(plan)], refs[len(plan):]
    inv_ref, swap_ref, cos_ref, sin_ref, sems = refs[:5]
    bufs, refs = refs[5:5 + count], refs[5 + count:]
    gain_bufs, rms_refs = refs[:len(turned)], refs[len(turned):]
    tokens, width = bufs[0].shape
    step = pl.program_id(0)

    @pl.when(step == 0)
    def _():
        pairs = [(inv_hbm, inv_ref)] + list(zip(sources, bufs)) + list(zip(gains, gain_bufs))
        copies = [pltpu.make_async_copy(a, b, sems.at[n]) for n, (a, b) in enumerate(pairs)]
        for copy in copies:
            copy.start()
        lane = lax.broadcasted_iota(jnp.int32, (HEAD_DIM, HEAD_DIM), 1)
        depth = lax.broadcasted_iota(jnp.int32, (HEAD_DIM, HEAD_DIM), 0)
        below = jnp.where((lane % 2 == 0) & (depth == lane + 1), -1.0, 0.0)
        above = jnp.where((lane % 2 == 1) & (depth == lane - 1), 1.0, 0.0)
        swap_ref[...] = (below + above).astype(BF16)
        copies[0].wait()
        token = block_ref[0] * tokens + lax.broadcasted_iota(jnp.int32, (tokens, HEAD_DIM), 0)
        pair = lax.broadcasted_iota(jnp.int32, (tokens, HEAD_DIM), 1) // 2
        sixth = HEAD_DIM // 6
        frame_pairs = (HEAD_DIM - 4 * sixth) // 2
        frame = token // (HGT * WID)
        row = (token // WID) % HGT
        column = token % WID
        coord = jnp.where(pair < frame_pairs, frame,
                          jnp.where(pair < frame_pairs + sixth, row, column)).astype(F32)
        angle = coord * inv_ref[...]
        cos_ref[...] = jnp.cos(angle)
        sin_ref[...] = jnp.sin(angle)
        for copy in copies[1:]:
            copy.wait()
        for src, dst in zip([bufs[n] for n in turned], rms_refs):
            total = jnp.zeros((tokens, HEAD_DIM), F32)
            for h in range(width // HEAD_DIM):
                x = src[:, h * HEAD_DIM:(h + 1) * HEAD_DIM].astype(F32)
                total = total + x * x
            mean = jnp.sum(total, axis=1, keepdims=True) / width
            dst[...] = jnp.broadcast_to(lax.rsqrt(mean + EPSILON), (tokens, HEAD_DIM))

    even = lax.broadcasted_iota(jnp.int32, (1, HEAD_DIM), 1) % 2 == 0

    def columns(n, head):
        return bufs[n][:, pl.ds(pl.multiple_of(head * HEAD_DIM, HEAD_DIM), HEAD_DIM)]

    def rotated(n, head):
        x = columns(n, head)
        xs = jnp.dot(x, swap_ref[...], preferred_element_type=F32)
        g = gain_bufs[turned.index(n)][pl.ds(head, 1), :]
        gs = jnp.where(even, pltpu.roll(g, HEAD_DIM - 1, 1), pltpu.roll(g, 1, 1))
        r = rms_refs[turned.index(n)][...]
        return (x.astype(F32) * r * g) * cos_ref[...] + (xs * r * gs) * sin_ref[...]

    for dst, (first, peers, heads, kinds) in zip(outs, plan):
        for peer in range(peers):
            for h in range(heads):
                head = first + (step * peers + peer) * heads + h
                for slot, kind in enumerate(kinds):
                    n = tensors.index(kind)
                    y = columns(n, head).astype(F32) if kind == "v" else rotated(n, head)
                    dst[peer, h, slot] = (y if kind == "k" else y.T).astype(BF16)


def prepare(steps, block, tensors, plan):
    kinds = tuple(tensors)
    tokens, width = tensors[kinds[0]][0].shape
    heads = width // HEAD_DIM
    inverse, _ = inverse_row()
    tile = (HEAD_DIM, tokens)
    gains = [tensors[k][1].reshape(heads, HEAD_DIM) for k in kinds if k != "v"]
    hbm = pl.BlockSpec(memory_space=pltpu.HBM)
    shapes = [(peers, count, len(slots)) + tile for _, peers, count, slots in plan]
    return pl.pallas_call(
        functools.partial(prep_kernel, tensors=kinds, plan=plan),
        grid=(steps,),
        in_specs=[pl.BlockSpec(memory_space=pltpu.SMEM)] + [hbm] * (1 + len(kinds) + len(gains)),
        out_specs=[pl.BlockSpec(shape, lambda i: (i, 0, 0, 0, 0)) for shape in shapes],
        out_shape=[jax.ShapeDtypeStruct((steps * shape[0],) + shape[1:], BF16)
                   for shape in shapes],
        scratch_shapes=[
            pltpu.VMEM((1, HEAD_DIM), F32),
            pltpu.VMEM((HEAD_DIM, HEAD_DIM), BF16),
            pltpu.VMEM((tokens, HEAD_DIM), F32),
            pltpu.VMEM((tokens, HEAD_DIM), F32),
            pltpu.SemaphoreType.DMA((1 + len(kinds) + len(gains),)),
        ] + [pltpu.VMEM((tokens, width), BF16) for _ in kinds]
        + [pltpu.VMEM((heads, HEAD_DIM), F32) for _ in gains]
        + [pltpu.VMEM((tokens, HEAD_DIM), F32) for _ in gains],
        compiler_params=pltpu.CompilerParams(vmem_limit_bytes=VMEM_BYTES),
    )(block, jnp.asarray(inverse)[None, :], *[tensors[k][0] for k in kinds], *gains)


def attend_kernel(*refs, sizes, resume, final, sub, together):
    count = len(sizes)
    q_ref, gate_ref = refs[:2]
    pieces = refs[2:2 + count]
    at = 2 + count
    if resume:
        stat_in, mixed_in = refs[at:at + 2]
        at += 2
    if final:
        o_ref = refs[at]
        at += 1
    else:
        stat_out, mixed_out = refs[at:at + 2]
        at += 2
    k_bufs, v_bufs, sems = refs[at:]
    group = pl.program_id(0)
    base = (group % 2) * together

    def loads(group, base):
        copies = []
        for h in range(together):
            offset = 0
            for i, size in enumerate(sizes):
                for j, buf in enumerate((k_bufs, v_bufs)):
                    copies.append(pltpu.make_async_copy(
                        pieces[i].at[:, group * together + h, j],
                        buf.at[base + h, pl.ds(offset, size)],
                        sems.at[base + h, 2 * i + j]))
                offset += size
        return copies

    @pl.when(pl.program_id(1) == 0)
    def _():
        @pl.when(group == 0)
        def _():
            for copy in loads(group, base):
                copy.start()

        @pl.when(group + 1 < pl.num_programs(0))
        def _():
            for copy in loads(group + 1, together - base):
                copy.start()

        for copy in loads(group, base):
            copy.wait()

    tiles = q_ref.shape[0]
    tq = tiles * HEAD_DIM
    key_tiles = sum(sizes)
    per_sub = sub // HEAD_DIM
    subs = key_tiles // per_sub

    def scaled(q):
        q = q.astype(F32) * SCALE
        high = q.astype(BF16)
        low = (q - high.astype(F32)).astype(BF16)
        return jnp.concatenate([high, low], axis=0)

    def scores(h, first, count, q_both):
        k = k_bufs[base + h, pl.ds(first, count)].reshape(count * HEAD_DIM, HEAD_DIM)
        return jnp.dot(jnp.concatenate([k, k], axis=1), q_both, preferred_element_type=F32)

    def weighted(h, first, count, e):
        v = jnp.concatenate([v_bufs[base + h, first + t] for t in range(count)], axis=1)
        return jnp.dot(v, e.astype(BF16), preferred_element_type=F32)

    def emit(h, tile, out):
        o_ref[tile, h] = (out * gate_ref[h]).astype(BF16)

    queries = [scaled(jnp.concatenate([q_ref[t, h, 0] for t in range(tiles)], axis=1))
               for h in range(together)]
    items = [(h, j) for h in range(together) for j in range(subs)]
    safe = None
    s = scores(0, 0, per_sub, queries[0])
    for n, (h, j) in enumerate(items):
        after = None
        if n + 1 < len(items):
            nh, nj = items[n + 1]
            after = scores(nh, nj * per_sub, per_sub, queries[nh])
        if j == 0:
            total = jnp.zeros((8, tq), F32)
            mixed = None
        e = jnp.exp2(s)
        total = total + jnp.sum(e.reshape(sub // 8, 8, tq), axis=0)
        d = weighted(h, j * per_sub, per_sub, e)
        mixed = d if mixed is None else mixed + d
        s = after
        if j + 1 < subs:
            continue
        if resume:
            total = total + stat_in[h, 8:16, :]
            mixed = mixed + mixed_in[h]
        row = jnp.sum(total, axis=0, keepdims=True)
        fine = (row > SMALLEST) & (row < LARGEST)
        if resume:
            fine = fine & (stat_in[h, 0:1, :] == 0.0)
        fine = jnp.where(fine, 1.0, 0.0)
        safe = fine if safe is None else jnp.minimum(safe, fine)
        if final:
            out = mixed / row
            for t in range(tiles):
                emit(h, t, out[:, t * HEAD_DIM:(t + 1) * HEAD_DIM])
        else:
            stat_out[h, 0:8, :] = jnp.zeros((8, tq), F32)
            stat_out[h, 8:16, :] = total
            mixed_out[h] = mixed

    @pl.when(jnp.min(safe) < 0.5)
    def _():
        def one_tile(n, carry):
            h = n // tiles
            t = n % tiles
            q_tile = scaled(q_ref[t, h, 0])
            lanes = pl.ds(pl.multiple_of(t * HEAD_DIM, HEAD_DIM), HEAD_DIM)
            if resume:
                state = (stat_in[h, 0:1, lanes], stat_in[h, 8:16, lanes], mixed_in[h, :, lanes])
            else:
                state = (jnp.full((1, HEAD_DIM), -1e30, F32), jnp.zeros((8, HEAD_DIM), F32),
                         jnp.zeros((HEAD_DIM, HEAD_DIM), F32))

            def one_block(j, state):
                peak, total, mixed = state
                s = scores(h, j * 8, 8, q_tile)
                new_peak = jnp.maximum(peak, jnp.max(s, axis=0, keepdims=True))
                shrink = jnp.exp2(peak - new_peak)
                e = jnp.exp2(s - new_peak)
                total = total * shrink + jnp.sum(e.reshape(HEAD_DIM, 8, HEAD_DIM), axis=0)
                return new_peak, total, mixed * shrink + weighted(h, j * 8, 8, e)

            peak, total, mixed = lax.fori_loop(0, key_tiles // 8, one_block, state)
            if final:
                emit(h, t, mixed / jnp.sum(total, axis=0, keepdims=True))
            else:
                stat_out[h, 0:8, lanes] = jnp.broadcast_to(peak, (8, HEAD_DIM))
                stat_out[h, 8:16, lanes] = total
                mixed_out[h, :, lanes] = mixed
            return carry

        lax.fori_loop(0, together * tiles, one_tile, 0)


def attend(query, gate, pieces, state=None, final=True, tq=1024, sub=512, together=1):
    sizes = tuple(p.shape[0] for p in pieces)
    query_tiles, heads = query.shape[:2]
    step = tq // HEAD_DIM
    keys = sum(sizes)
    slots = together * min(heads // together, 2)
    state_specs = [pl.BlockSpec((together, 16, tq), lambda h, i: (h, 0, i)),
                   pl.BlockSpec((together, HEAD_DIM, tq), lambda h, i: (h, 0, i))]
    state_shapes = [jax.ShapeDtypeStruct((heads, 16, query_tiles * HEAD_DIM), F32),
                    jax.ShapeDtypeStruct((heads, HEAD_DIM, query_tiles * HEAD_DIM), F32)]
    return pl.pallas_call(
        functools.partial(attend_kernel, sizes=sizes, resume=state is not None, final=final,
                          sub=sub, together=together),
        grid=(heads // together, query_tiles // step),
        in_specs=[
            pl.BlockSpec((step, together, 1, HEAD_DIM, HEAD_DIM), lambda h, i: (i, h, 0, 0, 0)),
            pl.BlockSpec((together, HEAD_DIM, HEAD_DIM), lambda h, i: (h, 0, 0)),
        ] + [pl.BlockSpec(memory_space=pl.ANY) for _ in pieces]
        + (state_specs if state is not None else []),
        out_specs=(pl.BlockSpec((step, together, HEAD_DIM, HEAD_DIM), lambda h, i: (i, h, 0, 0))
                   if final else state_specs),
        out_shape=(jax.ShapeDtypeStruct((query_tiles, heads, HEAD_DIM, HEAD_DIM), BF16)
                   if final else state_shapes),
        scratch_shapes=[
            pltpu.VMEM((slots, keys, HEAD_DIM, HEAD_DIM), BF16),
            pltpu.VMEM((slots, keys, HEAD_DIM, HEAD_DIM), BF16),
            pltpu.SemaphoreType.DMA((slots, 2 * len(pieces))),
        ],
        compiler_params=pltpu.CompilerParams(vmem_limit_bytes=VMEM_BYTES),
        cost_estimate=pl.CostEstimate(
            flops=8 * heads * query_tiles * keys * HEAD_DIM**3,
            transcendentals=heads * query_tiles * keys * HEAD_DIM**2,
            bytes_accessed=4 * heads * keys * HEAD_DIM**2,
        ),
    )(query, gate, *pieces, *(state or ()))


def post_kernel(*refs):
    o_ref = refs[-1]
    head = 0
    for src in refs[:-1]:
        for peer in range(src.shape[0]):
            for h in range(src.shape[1]):
                tile = src[peer, h].astype(F32).T.astype(BF16)
                o_ref[:, head * HEAD_DIM:(head + 1) * HEAD_DIM] = tile
                head += 1


def collect(*parts):
    tokens = parts[0].shape[-1]
    width = HEAD_DIM * sum(p.shape[0] * p.shape[1] for p in parts)
    return pl.pallas_call(
        post_kernel,
        out_shape=jax.ShapeDtypeStruct((tokens, width), BF16),
        compiler_params=pltpu.CompilerParams(vmem_limit_bytes=16 * 1024 * 1024),
        name="post",
    )(*parts)


def shift(axis, amount):
    size = lax.axis_size(axis)
    return [(i, (i + amount) % size) for i in range(size)]


def ring(low, high, axis):
    up_low = lax.ppermute(low, axis, shift(axis, 1))
    down_high = lax.ppermute(high, axis, shift(axis, -1))
    up_high = lax.ppermute(high, axis, shift(axis, 1))
    down_low = lax.ppermute(low, axis, shift(axis, -1))
    up_far = lax.ppermute(up_low, axis, shift(axis, 1))
    down_far = lax.ppermute(down_high, axis, shift(axis, -1))
    return [up_low, down_high, up_high, down_low], [up_far, down_far]


def gates(timestep, gate_base, time_weight, first, count):
    half_freq = FREQ // 2
    exponent = jnp.arange(half_freq, dtype=jnp.int32).astype(F32) / half_freq
    frequency = jnp.power(F32(10000.0), -exponent)
    phase = timestep.astype(F32)[:, None] * frequency[None, :]
    embedded = jnp.concatenate([jnp.cos(phase), jnp.sin(phase)], axis=1)
    start = first * HEAD_DIM
    width = count * HEAD_DIM
    weight = lax.dynamic_slice_in_dim(time_weight, start, width, 1)
    base = lax.dynamic_slice_in_dim(gate_base, start, width, 0)
    projected = jnp.dot(embedded, weight, precision=lax.Precision.HIGHEST,
                        preferred_element_type=F32)
    gate = base + projected[0]
    return jnp.broadcast_to(gate.reshape(count, HEAD_DIM, 1), (count, HEAD_DIM, HEAD_DIM))


def block_attention(queries, keys, values, query_gain, key_gain, timestep, gate_base, time_weight):
    x, z, y, core = (lax.axis_index(n) for n in ("x", "z", "y", "core"))
    block = (((x * 4 + z) * 4 + y) * 2 + core).reshape(1).astype(jnp.int32)
    wide, narrow = ("x", "z", "core"), ("x", "z")
    spread = functools.partial(lax.all_to_all, split_axis=0, concat_axis=0, tiled=True)
    gate_of = functools.partial(gates, timestep, gate_base, time_weight)
    q, k, v = (queries, query_gain), (keys, key_gain), (values, None)

    (a,) = prepare(4, block, {"q": q, "k": k, "v": v}, ((0, 4, 1, "qkv"),))
    (b,) = prepare(8, block, {"q": q, "k": k, "v": v}, ((16, 1, 3, "qkv"),))
    a = spread(a, wide)
    own_a = a[:, :, 1:]
    up_a = lax.ppermute(own_a, "y", shift("y", 1))
    down_a = lax.ppermute(own_a, "y", shift("y", -1))
    far_a = [lax.ppermute(up_a[:8], "y", shift("y", 1)),
             lax.ppermute(down_a[8:], "y", shift("y", -1))]
    b, a = lax.optimization_barrier((b, a))
    b = spread(b, narrow)
    own_b = [b[:4, :, 1:], b[4:, :, 1:]]
    near_b, far_b = ring(*own_b, "y")

    def other(parts):
        return [lax.ppermute(p, "core", shift("core", 1)) for p in parts]

    near_b = own_b + near_b + other(own_b) + other(near_b)
    far_b = far_b + other(far_b)
    gate_a = gate_of((x * 4 + z) * 2 + core, 1)
    gate_b = gate_of(16 + (x * 4 + z) * 3, 3)

    out_a = attend(a, gate_a, [own_a, up_a, down_a] + far_a)
    out_a = spread(out_a, wide)
    state = attend(b, gate_b, near_b, final=False)
    out_b = attend(b, gate_b, far_b, state)
    out_b = spread(out_b, narrow)
    return collect(out_a, out_b)


def solution(mesh):
    fine = Mesh(mesh.devices.reshape(2, 2, 4, 4, 2), ("expert", "x", "z", "y", "core"))
    rows = P(("expert", "x", "z", "y", "core"), None)
    part = P("expert")
    return jax.shard_map(
        block_attention,
        mesh=fine,
        in_specs=(rows, rows, rows, part, part, part, part, P("expert", None)),
        out_specs=rows,
        check_vma=False,
    )
```

```python
import functools
import math

import jax
import jax.numpy as jnp
import numpy as np
from jax import lax
from jax.experimental import pallas as pl
from jax.experimental.pallas import tpu as pltpu
from jax.sharding import Mesh
from jax.sharding import PartitionSpec as P


HEAD_DIM = 128
FREQ = 256
HGT = 32
WID = 32
EPSILON = 1e-06
LOG2E = 1.4426950408889634
SMALLEST = 2.0**-80
LARGEST = 2.0**100
SCALE = LOG2E / math.sqrt(HEAD_DIM)
VMEM_BYTES = 63 * 1024 * 1024
F32 = jnp.float32
BF16 = jnp.bfloat16


def inverse_row():
    half = HEAD_DIM // 2
    sixth = HEAD_DIM // 6
    frame = (HEAD_DIM - 4 * sixth) // 2
    j = np.arange(half)
    in_frame = j < frame
    in_row = (j >= frame) & (j < frame + sixth)
    local = np.where(in_frame, j, np.where(in_row, j - frame, j - frame - sixth))
    dims = np.where(in_frame, 2 * frame, 2 * sixth)
    inverse = np.power(10000.0, -2.0 * local / dims).astype(np.float32)
    kind = np.where(in_frame, 0, np.where(in_row, 1, 2))
    return np.repeat(inverse, 2), np.repeat(kind, 2)


def prep_kernel(block_ref, inv_hbm, *refs, tensors, plan):
    count = len(tensors)
    turned = [n for n, kind in enumerate(tensors) if kind != "v"]
    sources, refs = refs[:count], refs[count:]
    gains, refs = refs[:len(turned)], refs[len(turned):]
    outs, refs = refs[:len(plan)], refs[len(plan):]
    inv_ref, swap_ref, cos_ref, sin_ref, sems = refs[:5]
    bufs, refs = refs[5:5 + count], refs[5 + count:]
    gain_bufs, rms_refs = refs[:len(turned)], refs[len(turned):]
    tokens, width = bufs[0].shape
    step = pl.program_id(0)

    @pl.when(step == 0)
    def _():
        pairs = [(inv_hbm, inv_ref)] + list(zip(sources, bufs)) + list(zip(gains, gain_bufs))
        copies = [pltpu.make_async_copy(a, b, sems.at[n]) for n, (a, b) in enumerate(pairs)]
        for copy in copies:
            copy.start()
        lane = lax.broadcasted_iota(jnp.int32, (HEAD_DIM, HEAD_DIM), 1)
        depth = lax.broadcasted_iota(jnp.int32, (HEAD_DIM, HEAD_DIM), 0)
        below = jnp.where((lane % 2 == 0) & (depth == lane + 1), -1.0, 0.0)
        above = jnp.where((lane % 2 == 1) & (depth == lane - 1), 1.0, 0.0)
        swap_ref[...] = (below + above).astype(BF16)
        copies[0].wait()
        token = block_ref[0] * tokens + lax.broadcasted_iota(jnp.int32, (tokens, HEAD_DIM), 0)
        pair = lax.broadcasted_iota(jnp.int32, (tokens, HEAD_DIM), 1) // 2
        sixth = HEAD_DIM // 6
        frame_pairs = (HEAD_DIM - 4 * sixth) // 2
        frame = token // (HGT * WID)
        row = (token // WID) % HGT
        column = token % WID
        coord = jnp.where(pair < frame_pairs, frame,
                          jnp.where(pair < frame_pairs + sixth, row, column)).astype(F32)
        angle = coord * inv_ref[...]
        cos_ref[...] = jnp.cos(angle)
        sin_ref[...] = jnp.sin(angle)
        for copy in copies[1:]:
            copy.wait()
        for src, dst in zip([bufs[n] for n in turned], rms_refs):
            total = jnp.zeros((tokens, HEAD_DIM), F32)
            for h in range(width // HEAD_DIM):
                x = src[:, h * HEAD_DIM:(h + 1) * HEAD_DIM].astype(F32)
                total = total + x * x
            mean = jnp.sum(total, axis=1, keepdims=True) / width
            dst[...] = jnp.broadcast_to(lax.rsqrt(mean + EPSILON), (tokens, HEAD_DIM))

    even = lax.broadcasted_iota(jnp.int32, (1, HEAD_DIM), 1) % 2 == 0

    def columns(n, head):
        return bufs[n][:, pl.ds(pl.multiple_of(head * HEAD_DIM, HEAD_DIM), HEAD_DIM)]

    def rotated(n, head):
        x = columns(n, head)
        xs = jnp.dot(x, swap_ref[...], preferred_element_type=F32)
        g = gain_bufs[turned.index(n)][pl.ds(head, 1), :]
        gs = jnp.where(even, pltpu.roll(g, HEAD_DIM - 1, 1), pltpu.roll(g, 1, 1))
        r = rms_refs[turned.index(n)][...]
        return (x.astype(F32) * r * g) * cos_ref[...] + (xs * r * gs) * sin_ref[...]

    for dst, (peers, tiles) in zip(outs, plan):
        for peer in range(peers):
            for slot, (kind, stride, first) in enumerate(tiles):
                head = first + (step * peers + peer) * stride
                n = tensors.index(kind)
                y = columns(n, head).astype(F32) if kind == "v" else rotated(n, head)
                dst[peer, slot] = (y if kind == "k" else y.T).astype(BF16)


def prepare(steps, block, tensors, plan):
    kinds = tuple(tensors)
    tokens, width = tensors[kinds[0]][0].shape
    heads = width // HEAD_DIM
    inverse, _ = inverse_row()
    tile = (HEAD_DIM, tokens)
    gains = [tensors[k][1].reshape(heads, HEAD_DIM) for k in kinds if k != "v"]
    hbm = pl.BlockSpec(memory_space=pltpu.HBM)
    shapes = [(peers, len(tiles)) + tile for peers, tiles in plan]
    return pl.pallas_call(
        functools.partial(prep_kernel, tensors=kinds, plan=plan),
        grid=(steps,),
        in_specs=[pl.BlockSpec(memory_space=pltpu.SMEM)] + [hbm] * (1 + len(kinds) + len(gains)),
        out_specs=[pl.BlockSpec(shape, lambda i: (i, 0, 0, 0)) for shape in shapes],
        out_shape=[jax.ShapeDtypeStruct((steps * shape[0],) + shape[1:], BF16)
                   for shape in shapes],
        scratch_shapes=[
            pltpu.VMEM((1, HEAD_DIM), F32),
            pltpu.VMEM((HEAD_DIM, HEAD_DIM), BF16),
            pltpu.VMEM((tokens, HEAD_DIM), F32),
            pltpu.VMEM((tokens, HEAD_DIM), F32),
            pltpu.SemaphoreType.DMA((1 + len(kinds) + len(gains),)),
        ] + [pltpu.VMEM((tokens, width), BF16) for _ in kinds]
        + [pltpu.VMEM((heads, HEAD_DIM), F32) for _ in gains]
        + [pltpu.VMEM((tokens, HEAD_DIM), F32) for _ in gains],
        compiler_params=pltpu.CompilerParams(vmem_limit_bytes=VMEM_BYTES),
    )(block, jnp.asarray(inverse)[None, :], *[tensors[k][0] for k in kinds], *gains)


def attend_kernel(*refs, sizes, resume, final, sub, together):
    count = len(sizes)
    q_ref, gate_ref = refs[:2]
    pieces = refs[2:2 + count]
    at = 2 + count
    if resume:
        stat_in, mixed_in = refs[at:at + 2]
        at += 2
    if final:
        o_ref = refs[at]
        at += 1
    else:
        stat_out, mixed_out = refs[at:at + 2]
        at += 2
    k_bufs, v_bufs, sems = refs[at:]
    group = pl.program_id(0)
    base = (group % 2) * together

    def loads(group, base):
        copies = []
        for h in range(together):
            offset = 0
            for i, size in enumerate(sizes):
                for j, buf in enumerate((k_bufs, v_bufs)):
                    copies.append(pltpu.make_async_copy(
                        pieces[i].at[:, group * together + h, j],
                        buf.at[base + h, pl.ds(offset, size)],
                        sems.at[base + h, 2 * i + j]))
                offset += size
        return copies

    @pl.when(pl.program_id(1) == 0)
    def _():
        @pl.when(group == 0)
        def _():
            for copy in loads(group, base):
                copy.start()

        @pl.when(group + 1 < pl.num_programs(0))
        def _():
            for copy in loads(group + 1, together - base):
                copy.start()

        for copy in loads(group, base):
            copy.wait()

    tiles = q_ref.shape[0]
    tq = tiles * HEAD_DIM
    key_tiles = sum(sizes)
    per_sub = sub // HEAD_DIM
    subs = key_tiles // per_sub

    def scaled(q):
        q = q.astype(F32) * SCALE
        high = q.astype(BF16)
        low = (q - high.astype(F32)).astype(BF16)
        return jnp.concatenate([high, low], axis=0)

    def scores(h, first, count, q_both):
        k = k_bufs[base + h, pl.ds(first, count)].reshape(count * HEAD_DIM, HEAD_DIM)
        return jnp.dot(jnp.concatenate([k, k], axis=1), q_both, preferred_element_type=F32)

    def weighted(h, first, count, e):
        v = jnp.concatenate([v_bufs[base + h, first + t] for t in range(count)], axis=1)
        return jnp.dot(v, e.astype(BF16), preferred_element_type=F32)

    def emit(h, tile, out):
        o_ref[tile, h] = (out * gate_ref[h]).astype(BF16)

    queries = [scaled(jnp.concatenate([q_ref[t, h, 0] for t in range(tiles)], axis=1))
               for h in range(together)]
    items = [(h, j) for h in range(together) for j in range(subs)]
    safe = None
    s = scores(0, 0, per_sub, queries[0])
    for n, (h, j) in enumerate(items):
        after = None
        if n + 1 < len(items):
            nh, nj = items[n + 1]
            after = scores(nh, nj * per_sub, per_sub, queries[nh])
        if j == 0:
            total = jnp.zeros((8, tq), F32)
            mixed = None
        e = jnp.exp2(s)
        total = total + jnp.sum(e.reshape(sub // 8, 8, tq), axis=0)
        d = weighted(h, j * per_sub, per_sub, e)
        mixed = d if mixed is None else mixed + d
        s = after
        if j + 1 < subs:
            continue
        if resume:
            total = total + stat_in[h, 8:16, :]
            mixed = mixed + mixed_in[h]
        row = jnp.sum(total, axis=0, keepdims=True)
        fine = (row > SMALLEST) & (row < LARGEST)
        if resume:
            fine = fine & (stat_in[h, 0:1, :] == 0.0)
        fine = jnp.where(fine, 1.0, 0.0)
        safe = fine if safe is None else jnp.minimum(safe, fine)
        if final:
            out = mixed / row
            for t in range(tiles):
                emit(h, t, out[:, t * HEAD_DIM:(t + 1) * HEAD_DIM])
        else:
            stat_out[h, 0:8, :] = jnp.zeros((8, tq), F32)
            stat_out[h, 8:16, :] = total
            mixed_out[h] = mixed

    @pl.when(jnp.min(safe) < 0.5)
    def _():
        def one_tile(n, carry):
            h = n // tiles
            t = n % tiles
            q_tile = scaled(q_ref[t, h, 0])
            lanes = pl.ds(pl.multiple_of(t * HEAD_DIM, HEAD_DIM), HEAD_DIM)
            if resume:
                state = (stat_in[h, 0:1, lanes], stat_in[h, 8:16, lanes], mixed_in[h, :, lanes])
            else:
                state = (jnp.full((1, HEAD_DIM), -1e30, F32), jnp.zeros((8, HEAD_DIM), F32),
                         jnp.zeros((HEAD_DIM, HEAD_DIM), F32))

            def one_block(j, state):
                peak, total, mixed = state
                s = scores(h, j * 8, 8, q_tile)
                new_peak = jnp.maximum(peak, jnp.max(s, axis=0, keepdims=True))
                shrink = jnp.exp2(peak - new_peak)
                e = jnp.exp2(s - new_peak)
                total = total * shrink + jnp.sum(e.reshape(HEAD_DIM, 8, HEAD_DIM), axis=0)
                return new_peak, total, mixed * shrink + weighted(h, j * 8, 8, e)

            peak, total, mixed = lax.fori_loop(0, key_tiles // 8, one_block, state)
            if final:
                emit(h, t, mixed / jnp.sum(total, axis=0, keepdims=True))
            else:
                stat_out[h, 0:8, lanes] = jnp.broadcast_to(peak, (8, HEAD_DIM))
                stat_out[h, 8:16, lanes] = total
                mixed_out[h, :, lanes] = mixed
            return carry

        lax.fori_loop(0, together * tiles, one_tile, 0)


def attend(query, gate, pieces, state=None, final=True, tq=1024, sub=512, together=1):
    sizes = tuple(p.shape[0] for p in pieces)
    query_tiles, heads = query.shape[:2]
    step = tq // HEAD_DIM
    keys = sum(sizes)
    slots = together * min(heads // together, 2)
    state_specs = [pl.BlockSpec((together, 16, tq), lambda h, i: (h, 0, i)),
                   pl.BlockSpec((together, HEAD_DIM, tq), lambda h, i: (h, 0, i))]
    state_shapes = [jax.ShapeDtypeStruct((heads, 16, query_tiles * HEAD_DIM), F32),
                    jax.ShapeDtypeStruct((heads, HEAD_DIM, query_tiles * HEAD_DIM), F32)]
    return pl.pallas_call(
        functools.partial(attend_kernel, sizes=sizes, resume=state is not None, final=final,
                          sub=sub, together=together),
        grid=(heads // together, query_tiles // step),
        in_specs=[
            pl.BlockSpec((step, together, 1, HEAD_DIM, HEAD_DIM), lambda h, i: (i, h, 0, 0, 0)),
            pl.BlockSpec((together, HEAD_DIM, HEAD_DIM), lambda h, i: (h, 0, 0)),
        ] + [pl.BlockSpec(memory_space=pl.ANY) for _ in pieces]
        + (state_specs if state is not None else []),
        out_specs=(pl.BlockSpec((step, together, HEAD_DIM, HEAD_DIM), lambda h, i: (i, h, 0, 0))
                   if final else state_specs),
        out_shape=(jax.ShapeDtypeStruct((query_tiles, heads, HEAD_DIM, HEAD_DIM), BF16)
                   if final else state_shapes),
        scratch_shapes=[
            pltpu.VMEM((slots, keys, HEAD_DIM, HEAD_DIM), BF16),
            pltpu.VMEM((slots, keys, HEAD_DIM, HEAD_DIM), BF16),
            pltpu.SemaphoreType.DMA((slots, 2 * len(pieces))),
        ],
        compiler_params=pltpu.CompilerParams(vmem_limit_bytes=VMEM_BYTES),
        cost_estimate=pl.CostEstimate(
            flops=8 * heads * query_tiles * keys * HEAD_DIM**3,
            transcendentals=heads * query_tiles * keys * HEAD_DIM**2,
            bytes_accessed=4 * heads * keys * HEAD_DIM**2,
        ),
    )(query, gate, *pieces, *(state or ()))


def post_kernel(*refs):
    o_ref = refs[-1]
    head = 0
    for src in refs[:-1]:
        for peer in range(src.shape[0]):
            for h in range(src.shape[1]):
                tile = src[peer, h].astype(F32).T.astype(BF16)
                o_ref[:, head * HEAD_DIM:(head + 1) * HEAD_DIM] = tile
                head += 1


def collect(*parts):
    tokens = parts[0].shape[-1]
    width = HEAD_DIM * sum(p.shape[0] * p.shape[1] for p in parts)
    return pl.pallas_call(
        post_kernel,
        out_shape=jax.ShapeDtypeStruct((tokens, width), BF16),
        compiler_params=pltpu.CompilerParams(vmem_limit_bytes=16 * 1024 * 1024),
        name="post",
    )(*parts)


def shift(axis, amount):
    size = lax.axis_size(axis)
    return [(i, (i + amount) % size) for i in range(size)]


def ring(low, high, axis):
    up_low = lax.ppermute(low, axis, shift(axis, 1))
    down_high = lax.ppermute(high, axis, shift(axis, -1))
    up_high = lax.ppermute(high, axis, shift(axis, 1))
    down_low = lax.ppermute(low, axis, shift(axis, -1))
    up_far = lax.ppermute(up_low, axis, shift(axis, 1))
    down_far = lax.ppermute(down_high, axis, shift(axis, -1))
    return [up_low, down_high, up_high, down_low], [up_far, down_far]


def gates(timestep, gate_base, time_weight, first, count):
    half_freq = FREQ // 2
    exponent = jnp.arange(half_freq, dtype=jnp.int32).astype(F32) / half_freq
    frequency = jnp.power(F32(10000.0), -exponent)
    phase = timestep.astype(F32)[:, None] * frequency[None, :]
    embedded = jnp.concatenate([jnp.cos(phase), jnp.sin(phase)], axis=1)
    start = first * HEAD_DIM
    width = count * HEAD_DIM
    weight = lax.dynamic_slice_in_dim(time_weight, start, width, 1)
    base = lax.dynamic_slice_in_dim(gate_base, start, width, 0)
    projected = jnp.dot(embedded, weight, precision=lax.Precision.HIGHEST,
                        preferred_element_type=F32)
    gate = base + projected[0]
    return jnp.broadcast_to(gate.reshape(count, HEAD_DIM, 1), (count, HEAD_DIM, HEAD_DIM))


def block_attention(queries, keys, values, query_gain, key_gain, timestep, gate_base, time_weight):
    x, z, y, core = (lax.axis_index(n) for n in ("x", "z", "y", "core"))
    block = (((x * 4 + z) * 4 + y) * 2 + core).reshape(1).astype(jnp.int32)
    wide, narrow = ("x", "z", "core"), ("x", "z")
    spread = functools.partial(lax.all_to_all, split_axis=0, concat_axis=0, tiled=True)
    gate_of = functools.partial(gates, timestep, gate_base, time_weight)
    q, k, v = (queries, query_gain), (keys, key_gain), (values, None)

    key_values = tuple((kind, 3, 16 + h) for h in range(3) for kind in "kv")
    (a,) = prepare(4, block, {"k": k, "v": v}, ((4, (("k", 1, 0), ("v", 1, 0))),))
    b, b_query = prepare(8, block, {"q": q, "k": k, "v": v}, (
        (1, key_values + (("q", 2, 0), ("q", 2, 1))),
        (1, tuple(("q", 3, 16 + h) for h in range(3))),
    ))
    own_a = spread(a, wide).reshape(16, 1, 2, HEAD_DIM, -1)
    up_a = lax.ppermute(own_a, "y", shift("y", 1))
    down_a = lax.ppermute(own_a, "y", shift("y", -1))
    far_a = [lax.ppermute(up_a[:8], "y", shift("y", 1)),
             lax.ppermute(down_a[8:], "y", shift("y", -1))]
    b, own_a = lax.optimization_barrier((b, own_a))
    b = spread(b, narrow)
    own_b = [b[:4, :6].reshape(4, 3, 2, HEAD_DIM, -1), b[4:, :6].reshape(4, 3, 2, HEAD_DIM, -1)]
    near_b, far_b = ring(*own_b, "y")
    b_query, b = lax.optimization_barrier((b_query, b))
    b_query = spread(b_query, narrow).reshape(8, 3, 1, HEAD_DIM, -1)
    mine = lax.dynamic_slice_in_dim(b, 6 + core, 1, 1)
    sent = lax.dynamic_slice_in_dim(b, 7 - core, 1, 1)
    a_query = jnp.concatenate([mine, lax.ppermute(sent, "core", shift("core", 1))], axis=0)
    a_query = a_query.reshape(16, 1, 1, HEAD_DIM, -1)

    def other(parts):
        return [lax.ppermute(p, "core", shift("core", 1)) for p in parts]

    near_b = (own_b + near_b + other(own_b) + other(near_b[:2])
              + other(near_b[2:]))
    far_b = far_b + other(far_b)
    gate_a = gate_of((x * 4 + z) * 2 + core, 1)
    gate_b = gate_of(16 + (x * 4 + z) * 3, 3)

    out_a = attend(a_query, gate_a, [own_a, up_a, down_a] + far_a)
    out_a = out_a.reshape(2, 8, HEAD_DIM, -1)
    out_a = jnp.where(core == 0, out_a, out_a[::-1]).transpose(1, 0, 2, 3)
    out_a = spread(out_a.reshape(16, 1, HEAD_DIM, -1), wide)
    state = attend(b_query, gate_b, near_b, final=False)
    out_b = attend(b_query, gate_b, far_b, state)
    out_b = spread(out_b, narrow)
    return collect(out_a, out_b)


def solution(mesh):
    fine = Mesh(mesh.devices.reshape(2, 2, 4, 4, 2), ("expert", "x", "z", "y", "core"))
    rows = P(("expert", "x", "z", "y", "core"), None)
    part = P("expert")
    return jax.shard_map(
        block_attention,
        mesh=fine,
        in_specs=(rows, rows, rows, part, part, part, part, P("expert", None)),
        out_specs=rows,
        check_vma=False,
    )
```

```python
import functools
import math

import jax
import jax.numpy as jnp
import numpy as np
from jax import lax
from jax.experimental import pallas as pl
from jax.experimental.pallas import tpu as pltpu
from jax.sharding import Mesh
from jax.sharding import PartitionSpec as P


HEAD_DIM = 128
FREQ = 256
HGT = 32
WID = 32
EPSILON = 1e-06
LOG2E = 1.4426950408889634
SMALLEST = 2.0**-80
LARGEST = 2.0**100
SCALE = LOG2E / math.sqrt(HEAD_DIM)
VMEM_BYTES = 63 * 1024 * 1024
F32 = jnp.float32
BF16 = jnp.bfloat16


def inverse_row():
    half = HEAD_DIM // 2
    sixth = HEAD_DIM // 6
    frame = (HEAD_DIM - 4 * sixth) // 2
    j = np.arange(half)
    in_frame = j < frame
    in_row = (j >= frame) & (j < frame + sixth)
    local = np.where(in_frame, j, np.where(in_row, j - frame, j - frame - sixth))
    dims = np.where(in_frame, 2 * frame, 2 * sixth)
    inverse = np.power(10000.0, -2.0 * local / dims).astype(np.float32)
    kind = np.where(in_frame, 0, np.where(in_row, 1, 2))
    return np.repeat(inverse, 2), np.repeat(kind, 2)


def prep_kernel(block_ref, inv_hbm, *refs, tensors, plan):
    count = len(tensors)
    turned = [n for n, kind in enumerate(tensors) if kind != "v"]
    sources, refs = refs[:count], refs[count:]
    gains, refs = refs[:len(turned)], refs[len(turned):]
    outs, refs = refs[:len(plan)], refs[len(plan):]
    inv_ref, swap_ref, cos_ref, sin_ref, sems = refs[:5]
    bufs, refs = refs[5:5 + count], refs[5 + count:]
    gain_bufs, rms_refs = refs[:len(turned)], refs[len(turned):]
    tokens, width = bufs[0].shape
    step = pl.program_id(0)

    @pl.when(step == 0)
    def _():
        pairs = [(inv_hbm, inv_ref)] + list(zip(sources, bufs)) + list(zip(gains, gain_bufs))
        copies = [pltpu.make_async_copy(a, b, sems.at[n]) for n, (a, b) in enumerate(pairs)]
        for copy in copies:
            copy.start()
        lane = lax.broadcasted_iota(jnp.int32, (HEAD_DIM, HEAD_DIM), 1)
        depth = lax.broadcasted_iota(jnp.int32, (HEAD_DIM, HEAD_DIM), 0)
        below = jnp.where((lane % 2 == 0) & (depth == lane + 1), -1.0, 0.0)
        above = jnp.where((lane % 2 == 1) & (depth == lane - 1), 1.0, 0.0)
        swap_ref[...] = (below + above).astype(BF16)
        copies[0].wait()
        token = block_ref[0] * tokens + lax.broadcasted_iota(jnp.int32, (tokens, HEAD_DIM), 0)
        pair = lax.broadcasted_iota(jnp.int32, (tokens, HEAD_DIM), 1) // 2
        sixth = HEAD_DIM // 6
        frame_pairs = (HEAD_DIM - 4 * sixth) // 2
        frame = token // (HGT * WID)
        row = (token // WID) % HGT
        column = token % WID
        coord = jnp.where(pair < frame_pairs, frame,
                          jnp.where(pair < frame_pairs + sixth, row, column)).astype(F32)
        angle = coord * inv_ref[...]
        cos_ref[...] = jnp.cos(angle)
        sin_ref[...] = jnp.sin(angle)
        for copy in copies[1:]:
            copy.wait()
        for src, dst in zip([bufs[n] for n in turned], rms_refs):
            total = jnp.zeros((tokens, HEAD_DIM), F32)
            for h in range(width // HEAD_DIM):
                x = src[:, h * HEAD_DIM:(h + 1) * HEAD_DIM].astype(F32)
                total = total + x * x
            mean = jnp.sum(total, axis=1, keepdims=True) / width
            dst[...] = jnp.broadcast_to(lax.rsqrt(mean + EPSILON), (tokens, HEAD_DIM))

    even = lax.broadcasted_iota(jnp.int32, (1, HEAD_DIM), 1) % 2 == 0

    def columns(n, head):
        return bufs[n][:, pl.ds(pl.multiple_of(head * HEAD_DIM, HEAD_DIM), HEAD_DIM)]

    def rotated(n, head):
        x = columns(n, head)
        xs = jnp.dot(x, swap_ref[...], preferred_element_type=F32)
        g = gain_bufs[turned.index(n)][pl.ds(head, 1), :]
        gs = jnp.where(even, pltpu.roll(g, HEAD_DIM - 1, 1), pltpu.roll(g, 1, 1))
        r = rms_refs[turned.index(n)][...]
        return (x.astype(F32) * r * g) * cos_ref[...] + (xs * r * gs) * sin_ref[...]

    for dst, (peers, tiles) in zip(outs, plan):
        for peer in range(peers):
            for slot, (kind, stride, first) in enumerate(tiles):
                head = first + (step * peers + peer) * stride
                n = tensors.index(kind)
                y = columns(n, head).astype(F32) if kind == "v" else rotated(n, head)
                dst[peer, slot] = (y if kind == "k" else y.T).astype(BF16)


def prepare(steps, block, tensors, plan):
    kinds = tuple(tensors)
    tokens, width = tensors[kinds[0]][0].shape
    heads = width // HEAD_DIM
    inverse, _ = inverse_row()
    tile = (HEAD_DIM, tokens)
    gains = [tensors[k][1].reshape(heads, HEAD_DIM) for k in kinds if k != "v"]
    hbm = pl.BlockSpec(memory_space=pltpu.HBM)
    shapes = [(peers, len(tiles)) + tile for peers, tiles in plan]
    return pl.pallas_call(
        functools.partial(prep_kernel, tensors=kinds, plan=plan),
        grid=(steps,),
        in_specs=[pl.BlockSpec(memory_space=pltpu.SMEM)] + [hbm] * (1 + len(kinds) + len(gains)),
        out_specs=[pl.BlockSpec(shape, lambda i: (i, 0, 0, 0)) for shape in shapes],
        out_shape=[jax.ShapeDtypeStruct((steps * shape[0],) + shape[1:], BF16)
                   for shape in shapes],
        scratch_shapes=[
            pltpu.VMEM((1, HEAD_DIM), F32),
            pltpu.VMEM((HEAD_DIM, HEAD_DIM), BF16),
            pltpu.VMEM((tokens, HEAD_DIM), F32),
            pltpu.VMEM((tokens, HEAD_DIM), F32),
            pltpu.SemaphoreType.DMA((1 + len(kinds) + len(gains),)),
        ] + [pltpu.VMEM((tokens, width), BF16) for _ in kinds]
        + [pltpu.VMEM((heads, HEAD_DIM), F32) for _ in gains]
        + [pltpu.VMEM((tokens, HEAD_DIM), F32) for _ in gains],
        compiler_params=pltpu.CompilerParams(vmem_limit_bytes=VMEM_BYTES),
    )(block, jnp.asarray(inverse)[None, :], *[tensors[k][0] for k in kinds], *gains)


def attend_kernel(*refs, sizes, resume, final, sub, together):
    count = len(sizes)
    q_ref, gate_ref = refs[:2]
    pieces = refs[2:2 + count]
    at = 2 + count
    if resume:
        stat_in, mixed_in = refs[at:at + 2]
        at += 2
    if final:
        o_ref = refs[at]
        at += 1
    else:
        stat_out, mixed_out = refs[at:at + 2]
        at += 2
    k_bufs, v_bufs, sems = refs[at:]
    group = pl.program_id(0)
    base = (group % 2) * together

    def loads(group, base):
        copies = []
        for h in range(together):
            offset = 0
            for i, size in enumerate(sizes):
                for j, buf in enumerate((k_bufs, v_bufs)):
                    copies.append(pltpu.make_async_copy(
                        pieces[i].at[:, group * together + h, j],
                        buf.at[base + h, pl.ds(offset, size)],
                        sems.at[base + h, 2 * i + j]))
                offset += size
        return copies

    @pl.when(pl.program_id(1) == 0)
    def _():
        @pl.when(group == 0)
        def _():
            for copy in loads(group, base):
                copy.start()

        @pl.when(group + 1 < pl.num_programs(0))
        def _():
            for copy in loads(group + 1, together - base):
                copy.start()

        for copy in loads(group, base):
            copy.wait()

    tiles = q_ref.shape[0]
    tq = tiles * HEAD_DIM
    key_tiles = sum(sizes)
    per_sub = sub // HEAD_DIM
    subs = key_tiles // per_sub

    def scaled(q):
        q = q.astype(F32) * SCALE
        high = q.astype(BF16)
        low = (q - high.astype(F32)).astype(BF16)
        return jnp.concatenate([high, low], axis=0)

    def scores(h, first, count, q_both):
        k = k_bufs[base + h, pl.ds(first, count)].reshape(count * HEAD_DIM, HEAD_DIM)
        return jnp.dot(jnp.concatenate([k, k], axis=1), q_both, preferred_element_type=F32)

    def weighted(h, first, count, e):
        v = jnp.concatenate([v_bufs[base + h, first + t] for t in range(count)], axis=1)
        return jnp.dot(v, e.astype(BF16), preferred_element_type=F32)

    def emit(h, tile, out):
        o_ref[tile, h] = (out * gate_ref[h]).astype(BF16)

    queries = [scaled(jnp.concatenate([q_ref[t, h, 0] for t in range(tiles)], axis=1))
               for h in range(together)]
    items = [(h, j) for h in range(together) for j in range(subs)]
    safe = None
    s = scores(0, 0, per_sub, queries[0])
    for n, (h, j) in enumerate(items):
        after = None
        if n + 1 < len(items):
            nh, nj = items[n + 1]
            after = scores(nh, nj * per_sub, per_sub, queries[nh])
        if j == 0:
            total = jnp.zeros((8, tq), F32)
            mixed = None
        e = jnp.exp2(s)
        total = total + jnp.sum(e.reshape(sub // 8, 8, tq), axis=0)
        d = weighted(h, j * per_sub, per_sub, e)
        mixed = d if mixed is None else mixed + d
        s = after
        if j + 1 < subs:
            continue
        if resume:
            total = total + stat_in[h, 8:16, :]
            mixed = mixed + mixed_in[h]
        row = jnp.sum(total, axis=0, keepdims=True)
        fine = (row > SMALLEST) & (row < LARGEST)
        if resume:
            fine = fine & (stat_in[h, 0:1, :] == 0.0)
        fine = jnp.where(fine, 1.0, 0.0)
        safe = fine if safe is None else jnp.minimum(safe, fine)
        if final:
            out = mixed / row
            for t in range(tiles):
                emit(h, t, out[:, t * HEAD_DIM:(t + 1) * HEAD_DIM])
        else:
            stat_out[h, 0:8, :] = jnp.zeros((8, tq), F32)
            stat_out[h, 8:16, :] = total
            mixed_out[h] = mixed

    @pl.when(jnp.min(safe) < 0.5)
    def _():
        def one_tile(n, carry):
            h = n // tiles
            t = n % tiles
            q_tile = scaled(q_ref[t, h, 0])
            lanes = pl.ds(pl.multiple_of(t * HEAD_DIM, HEAD_DIM), HEAD_DIM)
            if resume:
                state = (stat_in[h, 0:1, lanes], stat_in[h, 8:16, lanes], mixed_in[h, :, lanes])
            else:
                state = (jnp.full((1, HEAD_DIM), -1e30, F32), jnp.zeros((8, HEAD_DIM), F32),
                         jnp.zeros((HEAD_DIM, HEAD_DIM), F32))

            def one_block(j, state):
                peak, total, mixed = state
                s = scores(h, j * 8, 8, q_tile)
                new_peak = jnp.maximum(peak, jnp.max(s, axis=0, keepdims=True))
                shrink = jnp.exp2(peak - new_peak)
                e = jnp.exp2(s - new_peak)
                total = total * shrink + jnp.sum(e.reshape(HEAD_DIM, 8, HEAD_DIM), axis=0)
                return new_peak, total, mixed * shrink + weighted(h, j * 8, 8, e)

            peak, total, mixed = lax.fori_loop(0, key_tiles // 8, one_block, state)
            if final:
                emit(h, t, mixed / jnp.sum(total, axis=0, keepdims=True))
            else:
                stat_out[h, 0:8, lanes] = jnp.broadcast_to(peak, (8, HEAD_DIM))
                stat_out[h, 8:16, lanes] = total
                mixed_out[h, :, lanes] = mixed
            return carry

        lax.fori_loop(0, together * tiles, one_tile, 0)


def attend(query, gate, pieces, state=None, final=True, tq=1024, sub=512, together=1):
    sizes = tuple(p.shape[0] for p in pieces)
    query_tiles, heads = query.shape[:2]
    step = tq // HEAD_DIM
    keys = sum(sizes)
    slots = together * min(heads // together, 2)
    state_specs = [pl.BlockSpec((together, 16, tq), lambda h, i: (h, 0, i)),
                   pl.BlockSpec((together, HEAD_DIM, tq), lambda h, i: (h, 0, i))]
    state_shapes = [jax.ShapeDtypeStruct((heads, 16, query_tiles * HEAD_DIM), F32),
                    jax.ShapeDtypeStruct((heads, HEAD_DIM, query_tiles * HEAD_DIM), F32)]
    return pl.pallas_call(
        functools.partial(attend_kernel, sizes=sizes, resume=state is not None, final=final,
                          sub=sub, together=together),
        grid=(heads // together, query_tiles // step),
        in_specs=[
            pl.BlockSpec((step, together, 1, HEAD_DIM, HEAD_DIM), lambda h, i: (i, h, 0, 0, 0)),
            pl.BlockSpec((together, HEAD_DIM, HEAD_DIM), lambda h, i: (h, 0, 0)),
        ] + [pl.BlockSpec(memory_space=pl.ANY) for _ in pieces]
        + (state_specs if state is not None else []),
        out_specs=(pl.BlockSpec((step, together, HEAD_DIM, HEAD_DIM), lambda h, i: (i, h, 0, 0))
                   if final else state_specs),
        out_shape=(jax.ShapeDtypeStruct((query_tiles, heads, HEAD_DIM, HEAD_DIM), BF16)
                   if final else state_shapes),
        scratch_shapes=[
            pltpu.VMEM((slots, keys, HEAD_DIM, HEAD_DIM), BF16),
            pltpu.VMEM((slots, keys, HEAD_DIM, HEAD_DIM), BF16),
            pltpu.SemaphoreType.DMA((slots, 2 * len(pieces))),
        ],
        compiler_params=pltpu.CompilerParams(vmem_limit_bytes=VMEM_BYTES),
        cost_estimate=pl.CostEstimate(
            flops=8 * heads * query_tiles * keys * HEAD_DIM**3,
            transcendentals=heads * query_tiles * keys * HEAD_DIM**2,
            bytes_accessed=4 * heads * keys * HEAD_DIM**2,
        ),
    )(query, gate, *pieces, *(state or ()))


def post_kernel(*refs):
    o_ref = refs[-1]
    head = 0
    for src in refs[:-1]:
        for peer in range(src.shape[0]):
            for h in range(src.shape[1]):
                tile = src[peer, h].astype(F32).T.astype(BF16)
                o_ref[:, head * HEAD_DIM:(head + 1) * HEAD_DIM] = tile
                head += 1


def collect(*parts):
    tokens = parts[0].shape[-1]
    width = HEAD_DIM * sum(p.shape[0] * p.shape[1] for p in parts)
    return pl.pallas_call(
        post_kernel,
        out_shape=jax.ShapeDtypeStruct((tokens, width), BF16),
        compiler_params=pltpu.CompilerParams(vmem_limit_bytes=16 * 1024 * 1024),
        name="post",
    )(*parts)


def shift(axis, amount):
    size = lax.axis_size(axis)
    return [(i, (i + amount) % size) for i in range(size)]


def opposed(amount):
    steps = (amount, -amount)
    return [(2 * y + c, 2 * ((y + steps[c]) % 4) + c) for y in range(4) for c in range(2)]


def ring(low, high, axis):
    up_low = lax.ppermute(low, axis, shift(axis, 1))
    down_high = lax.ppermute(high, axis, shift(axis, -1))
    up_high = lax.ppermute(high, axis, shift(axis, 1))
    down_low = lax.ppermute(low, axis, shift(axis, -1))
    up_far = lax.ppermute(up_low, axis, shift(axis, 1))
    down_far = lax.ppermute(down_high, axis, shift(axis, -1))
    return [up_low, down_high, up_high, down_low], [up_far, down_far]


def gates(timestep, gate_base, time_weight, first, count):
    half_freq = FREQ // 2
    exponent = jnp.arange(half_freq, dtype=jnp.int32).astype(F32) / half_freq
    frequency = jnp.power(F32(10000.0), -exponent)
    phase = timestep.astype(F32)[:, None] * frequency[None, :]
    embedded = jnp.concatenate([jnp.cos(phase), jnp.sin(phase)], axis=1)
    start = first * HEAD_DIM
    width = count * HEAD_DIM
    weight = lax.dynamic_slice_in_dim(time_weight, start, width, 1)
    base = lax.dynamic_slice_in_dim(gate_base, start, width, 0)
    projected = jnp.dot(embedded, weight, precision=lax.Precision.HIGHEST,
                        preferred_element_type=F32)
    gate = base + projected[0]
    return jnp.broadcast_to(gate.reshape(count, HEAD_DIM, 1), (count, HEAD_DIM, HEAD_DIM))


def block_attention(queries, keys, values, query_gain, key_gain, timestep, gate_base, time_weight):
    x, z, y, core = (lax.axis_index(n) for n in ("x", "z", "y", "core"))
    block = (((x * 4 + z) * 4 + y) * 2 + core).reshape(1).astype(jnp.int32)
    wide, narrow = ("x", "z", "core"), ("x", "z")
    spread = functools.partial(lax.all_to_all, split_axis=0, concat_axis=0, tiled=True)
    gate_of = functools.partial(gates, timestep, gate_base, time_weight)
    q, k, v = (queries, query_gain), (keys, key_gain), (values, None)

    key_values = tuple((kind, 3, 16 + h) for h in range(3) for kind in "kv")
    (a,) = prepare(4, block, {"k": k, "v": v}, ((4, (("k", 1, 0), ("v", 1, 0))),))
    b, b_query = prepare(8, block, {"q": q, "k": k, "v": v}, (
        (1, key_values + (("q", 2, 0), ("q", 2, 1))),
        (1, tuple(("q", 3, 16 + h) for h in range(3))),
    ))
    own_a = spread(a, wide).reshape(16, 1, 2, HEAD_DIM, -1)
    first_a = lax.ppermute(own_a, ("y", "core"), opposed(1))
    second_a = lax.ppermute(own_a, ("y", "core"), opposed(-1))
    far_a = lax.ppermute(first_a, ("y", "core"), opposed(1))
    b, own_a = lax.optimization_barrier((b, own_a))
    b = spread(b, narrow)
    own_b = [b[:4, :6].reshape(4, 3, 2, HEAD_DIM, -1), b[4:, :6].reshape(4, 3, 2, HEAD_DIM, -1)]
    near_b, far_b = ring(*own_b, "y")
    b_query, b = lax.optimization_barrier((b_query, b))
    b_query = spread(b_query, narrow).reshape(8, 3, 1, HEAD_DIM, -1)
    mine = lax.dynamic_slice_in_dim(b, 6 + core, 1, 1)
    sent = lax.dynamic_slice_in_dim(b, 7 - core, 1, 1)
    a_query = jnp.concatenate([mine, lax.ppermute(sent, "core", shift("core", 1))], axis=0)
    a_query = a_query.reshape(16, 1, 1, HEAD_DIM, -1)

    def other(parts):
        return [lax.ppermute(p, "core", shift("core", 1)) for p in parts]

    far_b = other(near_b[2:]) + far_b + other(far_b)
    near_b = own_b + near_b + other(own_b) + other(near_b[:2])
    gate_a = gate_of((x * 4 + z) * 2 + core, 1)
    gate_b = gate_of(16 + (x * 4 + z) * 3, 3)

    out_a = attend(a_query, gate_a, [own_a, first_a, second_a, far_a])
    out_a = out_a.reshape(2, 8, HEAD_DIM, -1)
    out_a = jnp.where(core == 0, out_a, out_a[::-1]).transpose(1, 0, 2, 3)
    out_a = spread(out_a.reshape(16, 1, HEAD_DIM, -1), wide)
    state = attend(b_query, gate_b, near_b, final=False)
    out_b = attend(b_query, gate_b, far_b, state)
    out_b = spread(out_b, narrow)
    return collect(out_a, out_b)


def solution(mesh):
    fine = Mesh(mesh.devices.reshape(2, 2, 4, 4, 2), ("expert", "x", "z", "y", "core"))
    rows = P(("expert", "x", "z", "y", "core"), None)
    part = P("expert")
    return jax.shard_map(
        block_attention,
        mesh=fine,
        in_specs=(rows, rows, rows, part, part, part, part, P("expert", None)),
        out_specs=rows,
        check_vma=False,
    )
```

```python
import functools
import math

import jax
import jax.numpy as jnp
import numpy as np
from jax import lax
from jax.experimental import pallas as pl
from jax.experimental.pallas import tpu as pltpu
from jax.sharding import Mesh
from jax.sharding import PartitionSpec as P


HEAD_DIM = 128
FREQ = 256
HGT = 32
WID = 32
EPSILON = 1e-06
LOG2E = 1.4426950408889634
SMALLEST = 2.0**-80
LARGEST = 2.0**100
SCALE = LOG2E / math.sqrt(HEAD_DIM)
VMEM_BYTES = 63 * 1024 * 1024
F32 = jnp.float32
BF16 = jnp.bfloat16


def inverse_row():
    half = HEAD_DIM // 2
    sixth = HEAD_DIM // 6
    frame = (HEAD_DIM - 4 * sixth) // 2
    j = np.arange(half)
    in_frame = j < frame
    in_row = (j >= frame) & (j < frame + sixth)
    local = np.where(in_frame, j, np.where(in_row, j - frame, j - frame - sixth))
    dims = np.where(in_frame, 2 * frame, 2 * sixth)
    inverse = np.power(10000.0, -2.0 * local / dims).astype(np.float32)
    kind = np.where(in_frame, 0, np.where(in_row, 1, 2))
    return np.repeat(inverse, 2), np.repeat(kind, 2)


def prep_kernel(block_ref, inv_hbm, *refs, tensors, plan):
    count = len(tensors)
    turned = [n for n, kind in enumerate(tensors) if kind != "v"]
    sources, refs = refs[:count], refs[count:]
    gains, refs = refs[:len(turned)], refs[len(turned):]
    outs, refs = refs[:len(plan)], refs[len(plan):]
    inv_ref, swap_ref, cos_ref, sin_ref, sems = refs[:5]
    bufs, refs = refs[5:5 + count], refs[5 + count:]
    gain_bufs, rms_refs = refs[:len(turned)], refs[len(turned):]
    tokens, width = bufs[0].shape
    step = pl.program_id(0)

    @pl.when(step == 0)
    def _():
        pairs = [(inv_hbm, inv_ref)] + list(zip(sources, bufs)) + list(zip(gains, gain_bufs))
        copies = [pltpu.make_async_copy(a, b, sems.at[n]) for n, (a, b) in enumerate(pairs)]
        for copy in copies:
            copy.start()
        lane = lax.broadcasted_iota(jnp.int32, (HEAD_DIM, HEAD_DIM), 1)
        depth = lax.broadcasted_iota(jnp.int32, (HEAD_DIM, HEAD_DIM), 0)
        below = jnp.where((lane % 2 == 0) & (depth == lane + 1), -1.0, 0.0)
        above = jnp.where((lane % 2 == 1) & (depth == lane - 1), 1.0, 0.0)
        swap_ref[...] = (below + above).astype(BF16)
        copies[0].wait()
        token = block_ref[0] * tokens + lax.broadcasted_iota(jnp.int32, (tokens, HEAD_DIM), 0)
        pair = lax.broadcasted_iota(jnp.int32, (tokens, HEAD_DIM), 1) // 2
        sixth = HEAD_DIM // 6
        frame_pairs = (HEAD_DIM - 4 * sixth) // 2
        frame = token // (HGT * WID)
        row = (token // WID) % HGT
        column = token % WID
        coord = jnp.where(pair < frame_pairs, frame,
                          jnp.where(pair < frame_pairs + sixth, row, column)).astype(F32)
        angle = coord * inv_ref[...]
        cos_ref[...] = jnp.cos(angle)
        sin_ref[...] = jnp.sin(angle)
        for copy in copies[1:]:
            copy.wait()
        for src, dst in zip([bufs[n] for n in turned], rms_refs):
            total = jnp.zeros((tokens, HEAD_DIM), F32)
            for h in range(width // HEAD_DIM):
                x = src[:, h * HEAD_DIM:(h + 1) * HEAD_DIM].astype(F32)
                total = total + x * x
            mean = jnp.sum(total, axis=1, keepdims=True) / width
            dst[...] = jnp.broadcast_to(lax.rsqrt(mean + EPSILON), (tokens, HEAD_DIM))

    even = lax.broadcasted_iota(jnp.int32, (1, HEAD_DIM), 1) % 2 == 0

    def columns(n, head):
        return bufs[n][:, pl.ds(pl.multiple_of(head * HEAD_DIM, HEAD_DIM), HEAD_DIM)]

    def rotated(n, head):
        x = columns(n, head)
        xs = jnp.dot(x, swap_ref[...], preferred_element_type=F32)
        g = gain_bufs[turned.index(n)][pl.ds(head, 1), :]
        gs = jnp.where(even, pltpu.roll(g, HEAD_DIM - 1, 1), pltpu.roll(g, 1, 1))
        r = rms_refs[turned.index(n)][...]
        return (x.astype(F32) * r * g) * cos_ref[...] + (xs * r * gs) * sin_ref[...]

    for dst, (peers, tiles) in zip(outs, plan):
        for peer in range(peers):
            for slot, (kind, stride, first) in enumerate(tiles):
                head = first + (step * peers + peer) * stride
                n = tensors.index(kind)
                y = columns(n, head).astype(F32) if kind == "v" else rotated(n, head)
                dst[peer, slot] = (y if kind == "k" else y.T).astype(BF16)


def prepare(steps, block, tensors, plan):
    kinds = tuple(tensors)
    tokens, width = tensors[kinds[0]][0].shape
    heads = width // HEAD_DIM
    inverse, _ = inverse_row()
    tile = (HEAD_DIM, tokens)
    gains = [tensors[k][1].reshape(heads, HEAD_DIM) for k in kinds if k != "v"]
    hbm = pl.BlockSpec(memory_space=pltpu.HBM)
    shapes = [(peers, len(tiles)) + tile for peers, tiles in plan]
    return pl.pallas_call(
        functools.partial(prep_kernel, tensors=kinds, plan=plan),
        grid=(steps,),
        in_specs=[pl.BlockSpec(memory_space=pltpu.SMEM)] + [hbm] * (1 + len(kinds) + len(gains)),
        out_specs=[pl.BlockSpec(shape, lambda i: (i, 0, 0, 0)) for shape in shapes],
        out_shape=[jax.ShapeDtypeStruct((steps * shape[0],) + shape[1:], BF16)
                   for shape in shapes],
        scratch_shapes=[
            pltpu.VMEM((1, HEAD_DIM), F32),
            pltpu.VMEM((HEAD_DIM, HEAD_DIM), BF16),
            pltpu.VMEM((tokens, HEAD_DIM), F32),
            pltpu.VMEM((tokens, HEAD_DIM), F32),
            pltpu.SemaphoreType.DMA((1 + len(kinds) + len(gains),)),
        ] + [pltpu.VMEM((tokens, width), BF16) for _ in kinds]
        + [pltpu.VMEM((heads, HEAD_DIM), F32) for _ in gains]
        + [pltpu.VMEM((tokens, HEAD_DIM), F32) for _ in gains],
        compiler_params=pltpu.CompilerParams(vmem_limit_bytes=VMEM_BYTES),
    )(block, jnp.asarray(inverse)[None, :], *[tensors[k][0] for k in kinds], *gains)


def attend_kernel(*refs, sizes, resume, final, sub, together):
    count = len(sizes)
    q_ref, gate_ref = refs[:2]
    pieces = refs[2:2 + count]
    at = 2 + count
    if resume:
        stat_in, mixed_in = refs[at:at + 2]
        at += 2
    if final:
        o_ref = refs[at]
        at += 1
    else:
        stat_out, mixed_out = refs[at:at + 2]
        at += 2
    k_bufs, v_bufs, sems = refs[at:]
    group = pl.program_id(0)
    base = (group % 2) * together

    def loads(group, base):
        copies = []
        for h in range(together):
            offset = 0
            for i, size in enumerate(sizes):
                for j, buf in enumerate((k_bufs, v_bufs)):
                    copies.append(pltpu.make_async_copy(
                        pieces[i].at[:, group * together + h, j],
                        buf.at[base + h, pl.ds(offset, size)],
                        sems.at[base + h, 2 * i + j]))
                offset += size
        return copies

    @pl.when(pl.program_id(1) == 0)
    def _():
        @pl.when(group == 0)
        def _():
            for copy in loads(group, base):
                copy.start()

        @pl.when(group + 1 < pl.num_programs(0))
        def _():
            for copy in loads(group + 1, together - base):
                copy.start()

        for copy in loads(group, base):
            copy.wait()

    tiles = q_ref.shape[0]
    tq = tiles * HEAD_DIM
    key_tiles = sum(sizes)
    per_sub = sub // HEAD_DIM
    subs = key_tiles // per_sub

    def scaled(q):
        q = q.astype(F32) * SCALE
        high = q.astype(BF16)
        low = (q - high.astype(F32)).astype(BF16)
        return jnp.concatenate([high, low], axis=0)

    def scores(h, first, count, q_both):
        k = k_bufs[base + h, pl.ds(first, count)].reshape(count * HEAD_DIM, HEAD_DIM)
        return jnp.dot(jnp.concatenate([k, k], axis=1), q_both, preferred_element_type=F32)

    def weighted(h, first, count, e):
        v = jnp.concatenate([v_bufs[base + h, first + t] for t in range(count)], axis=1)
        return jnp.dot(v, e.astype(BF16), preferred_element_type=F32)

    def emit(h, tile, out):
        o_ref[tile, h] = (out * gate_ref[h]).astype(BF16)

    queries = [scaled(jnp.concatenate([q_ref[t, h, 0] for t in range(tiles)], axis=1))
               for h in range(together)]
    items = [(h, j) for h in range(together) for j in range(subs)]
    safe = None
    s = scores(0, 0, per_sub, queries[0])
    for n, (h, j) in enumerate(items):
        after = None
        if n + 1 < len(items):
            nh, nj = items[n + 1]
            after = scores(nh, nj * per_sub, per_sub, queries[nh])
        if j == 0:
            total = jnp.zeros((8, tq), F32)
            mixed = None
        e = jnp.exp2(s)
        total = total + jnp.sum(e.reshape(sub // 8, 8, tq), axis=0)
        d = weighted(h, j * per_sub, per_sub, e)
        mixed = d if mixed is None else mixed + d
        s = after
        if j + 1 < subs:
            continue
        if resume:
            total = total + stat_in[h, 8:16, :]
            mixed = mixed + mixed_in[h]
        row = jnp.sum(total, axis=0, keepdims=True)
        fine = (row > SMALLEST) & (row < LARGEST)
        if resume:
            fine = fine & (stat_in[h, 0:1, :] == 0.0)
        fine = jnp.where(fine, 1.0, 0.0)
        safe = fine if safe is None else jnp.minimum(safe, fine)
        if final:
            out = mixed / row
            for t in range(tiles):
                emit(h, t, out[:, t * HEAD_DIM:(t + 1) * HEAD_DIM])
        else:
            stat_out[h, 0:8, :] = jnp.zeros((8, tq), F32)
            stat_out[h, 8:16, :] = total
            mixed_out[h] = mixed

    @pl.when(jnp.min(safe) < 0.5)
    def _():
        def one_tile(n, carry):
            h = n // tiles
            t = n % tiles
            q_tile = scaled(q_ref[t, h, 0])
            lanes = pl.ds(pl.multiple_of(t * HEAD_DIM, HEAD_DIM), HEAD_DIM)
            if resume:
                state = (stat_in[h, 0:1, lanes], stat_in[h, 8:16, lanes], mixed_in[h, :, lanes])
            else:
                state = (jnp.full((1, HEAD_DIM), -1e30, F32), jnp.zeros((8, HEAD_DIM), F32),
                         jnp.zeros((HEAD_DIM, HEAD_DIM), F32))

            def one_block(j, state):
                peak, total, mixed = state
                s = scores(h, j * 8, 8, q_tile)
                new_peak = jnp.maximum(peak, jnp.max(s, axis=0, keepdims=True))
                shrink = jnp.exp2(peak - new_peak)
                e = jnp.exp2(s - new_peak)
                total = total * shrink + jnp.sum(e.reshape(HEAD_DIM, 8, HEAD_DIM), axis=0)
                return new_peak, total, mixed * shrink + weighted(h, j * 8, 8, e)

            peak, total, mixed = lax.fori_loop(0, key_tiles // 8, one_block, state)
            if final:
                emit(h, t, mixed / jnp.sum(total, axis=0, keepdims=True))
            else:
                stat_out[h, 0:8, lanes] = jnp.broadcast_to(peak, (8, HEAD_DIM))
                stat_out[h, 8:16, lanes] = total
                mixed_out[h, :, lanes] = mixed
            return carry

        lax.fori_loop(0, together * tiles, one_tile, 0)


def attend(query, gate, pieces, state=None, final=True, tq=1024, sub=512, together=1):
    sizes = tuple(p.shape[0] for p in pieces)
    query_tiles, heads = query.shape[:2]
    step = tq // HEAD_DIM
    keys = sum(sizes)
    slots = together * min(heads // together, 2)
    state_specs = [pl.BlockSpec((together, 16, tq), lambda h, i: (h, 0, i)),
                   pl.BlockSpec((together, HEAD_DIM, tq), lambda h, i: (h, 0, i))]
    state_shapes = [jax.ShapeDtypeStruct((heads, 16, query_tiles * HEAD_DIM), F32),
                    jax.ShapeDtypeStruct((heads, HEAD_DIM, query_tiles * HEAD_DIM), F32)]
    return pl.pallas_call(
        functools.partial(attend_kernel, sizes=sizes, resume=state is not None, final=final,
                          sub=sub, together=together),
        grid=(heads // together, query_tiles // step),
        in_specs=[
            pl.BlockSpec((step, together, 1, HEAD_DIM, HEAD_DIM), lambda h, i: (i, h, 0, 0, 0)),
            pl.BlockSpec((together, HEAD_DIM, HEAD_DIM), lambda h, i: (h, 0, 0)),
        ] + [pl.BlockSpec(memory_space=pl.ANY) for _ in pieces]
        + (state_specs if state is not None else []),
        out_specs=(pl.BlockSpec((step, together, HEAD_DIM, HEAD_DIM), lambda h, i: (i, h, 0, 0))
                   if final else state_specs),
        out_shape=(jax.ShapeDtypeStruct((query_tiles, heads, HEAD_DIM, HEAD_DIM), BF16)
                   if final else state_shapes),
        scratch_shapes=[
            pltpu.VMEM((slots, keys, HEAD_DIM, HEAD_DIM), BF16),
            pltpu.VMEM((slots, keys, HEAD_DIM, HEAD_DIM), BF16),
            pltpu.SemaphoreType.DMA((slots, 2 * len(pieces))),
        ],
        compiler_params=pltpu.CompilerParams(vmem_limit_bytes=VMEM_BYTES),
        cost_estimate=pl.CostEstimate(
            flops=8 * heads * query_tiles * keys * HEAD_DIM**3,
            transcendentals=heads * query_tiles * keys * HEAD_DIM**2,
            bytes_accessed=4 * heads * keys * HEAD_DIM**2,
        ),
    )(query, gate, *pieces, *(state or ()))


def post_kernel(*refs):
    o_ref = refs[-1]
    head = 0
    for src in refs[:-1]:
        for peer in range(src.shape[0]):
            for h in range(src.shape[1]):
                tile = src[peer, h].astype(F32).T.astype(BF16)
                o_ref[:, head * HEAD_DIM:(head + 1) * HEAD_DIM] = tile
                head += 1


def collect(*parts):
    tokens = parts[0].shape[-1]
    width = HEAD_DIM * sum(p.shape[0] * p.shape[1] for p in parts)
    return pl.pallas_call(
        post_kernel,
        out_shape=jax.ShapeDtypeStruct((tokens, width), BF16),
        compiler_params=pltpu.CompilerParams(vmem_limit_bytes=16 * 1024 * 1024),
        name="post",
    )(*parts)


def shift(axis, amount):
    size = lax.axis_size(axis)
    return [(i, (i + amount) % size) for i in range(size)]


def ring(low, high, axis):
    up_low = lax.ppermute(low, axis, shift(axis, 1))
    down_high = lax.ppermute(high, axis, shift(axis, -1))
    up_high = lax.ppermute(high, axis, shift(axis, 1))
    down_low = lax.ppermute(low, axis, shift(axis, -1))
    up_far = lax.ppermute(up_low, axis, shift(axis, 1))
    down_far = lax.ppermute(down_high, axis, shift(axis, -1))
    return [up_low, down_high, up_high, down_low], [up_far, down_far]


def gates(timestep, gate_base, time_weight, first, count):
    half_freq = FREQ // 2
    exponent = jnp.arange(half_freq, dtype=jnp.int32).astype(F32) / half_freq
    frequency = jnp.power(F32(10000.0), -exponent)
    phase = timestep.astype(F32)[:, None] * frequency[None, :]
    embedded = jnp.concatenate([jnp.cos(phase), jnp.sin(phase)], axis=1)
    start = first * HEAD_DIM
    width = count * HEAD_DIM
    weight = lax.dynamic_slice_in_dim(time_weight, start, width, 1)
    base = lax.dynamic_slice_in_dim(gate_base, start, width, 0)
    projected = jnp.dot(embedded, weight, precision=lax.Precision.HIGHEST,
                        preferred_element_type=F32)
    gate = base + projected[0]
    return jnp.broadcast_to(gate.reshape(count, HEAD_DIM, 1), (count, HEAD_DIM, HEAD_DIM))


def block_attention(queries, keys, values, query_gain, key_gain, timestep, gate_base, time_weight):
    x, z, y, core = (lax.axis_index(n) for n in ("x", "z", "y", "core"))
    block = (((x * 4 + z) * 4 + y) * 2 + core).reshape(1).astype(jnp.int32)
    wide, narrow = ("x", "z", "core"), ("x", "z")
    spread = functools.partial(lax.all_to_all, split_axis=0, concat_axis=0, tiled=True)
    gate_of = functools.partial(gates, timestep, gate_base, time_weight)
    q, k, v = (queries, query_gain), (keys, key_gain), (values, None)

    key_values = tuple((kind, 3, 16 + h) for h in range(3) for kind in "kv")
    (a,) = prepare(2, block, {"k": k, "v": v}, ((8, (("k", 1, 0), ("v", 1, 0))),))
    b, b_query = prepare(8, block, {"q": q, "k": k, "v": v}, (
        (1, key_values + (("q", 2, 0), ("q", 2, 1))),
        (1, tuple(("q", 3, 16 + h) for h in range(3))),
    ))
    own_a = spread(a, wide).reshape(16, 1, 2, HEAD_DIM, -1)
    up_a = lax.ppermute(own_a, "y", shift("y", 1))
    down_a = lax.ppermute(own_a, "y", shift("y", -1))
    far_a = [lax.ppermute(up_a[:8], "y", shift("y", 1)),
             lax.ppermute(down_a[8:], "y", shift("y", -1))]
    b, own_a = lax.optimization_barrier((b, own_a))
    b = spread(b, narrow)
    own_b = [b[:4, :6].reshape(4, 3, 2, HEAD_DIM, -1), b[4:, :6].reshape(4, 3, 2, HEAD_DIM, -1)]
    near_b, far_b = ring(*own_b, "y")
    b_query, b = lax.optimization_barrier((b_query, b))
    b_query = spread(b_query, narrow).reshape(8, 3, 1, HEAD_DIM, -1)
    mine = lax.dynamic_slice_in_dim(b, 6 + core, 1, 1)
    sent = lax.dynamic_slice_in_dim(b, 7 - core, 1, 1)
    a_query = jnp.concatenate([mine, lax.ppermute(sent, "core", shift("core", 1))], axis=0)
    a_query = a_query.reshape(16, 1, 1, HEAD_DIM, -1)

    def other(parts):
        return [lax.ppermute(p, "core", shift("core", 1)) for p in parts]

    far_b = other(near_b[2:]) + far_b + other(far_b)
    near_b = own_b + near_b + other(own_b) + other(near_b[:2])
    gate_a = gate_of((x * 4 + z) * 2 + core, 1)
    gate_b = gate_of(16 + (x * 4 + z) * 3, 3)

    out_a = attend(a_query, gate_a, [own_a, up_a, down_a] + far_a)
    out_a = out_a.reshape(2, 8, HEAD_DIM, -1)
    out_a = jnp.where(core == 0, out_a, out_a[::-1]).transpose(1, 0, 2, 3)
    out_a = spread(out_a.reshape(16, 1, HEAD_DIM, -1), wide)
    state = attend(b_query, gate_b, near_b, final=False)
    out_b = attend(b_query, gate_b, far_b, state)
    out_b = spread(out_b, narrow)
    return collect(out_a, out_b)


def solution(mesh):
    fine = Mesh(mesh.devices.reshape(2, 2, 4, 4, 2), ("expert", "x", "z", "y", "core"))
    rows = P(("expert", "x", "z", "y", "core"), None)
    part = P("expert")
    return jax.shard_map(
        block_attention,
        mesh=fine,
        in_specs=(rows, rows, rows, part, part, part, part, P("expert", None)),
        out_specs=rows,
        check_vma=False,
    )
```
